128 devices in a mesh: node: 16 (over z, y), dev: 8 (over x, core).
Axes of the slice: x: 4, y: 4, z: 4, core: 2. Of those that a mesh axis runs over, the one named last changes fastest.
Arguments:
- tokens: bfloat16 [8192, 5120], P(('node', 'dev')), may hold values from -6 to 6
- node_ids: int32 [8192, 3], P(('node', 'dev')), may hold values from 0 to 15, all different within a row; in each aligned block of 64 rows (0 to 63, 64 to 127, ...) at most 13 rows name the same one
- expert_pick: int32 [8192, 6], P(('node', 'dev')), may hold values from 0 to 8, all different within a row
- gate_share: bfloat16 [8192, 6], P(('node', 'dev')), may hold values from 0.099609375 to 1
- gate_proj: bfloat16 [48, 1536, 5120], P('node', 'dev'), may hold values from -0.078125 to 0.078125
- up_proj: bfloat16 [48, 1536, 5120], P('node', 'dev'), may hold values from -0.078125 to 0.078125
- down_proj: bfloat16 [48, 1536, 5120], P('node', 'dev'), may hold values from -0.15625 to 0.15625
Outputs:
- moe_out: bfloat16 [8192, 5120], P(('node', 'dev'))
The draws below stay inside these ranges and needn't reach their ends.
Inputs may be any that keep to these rules, and one draw needn't show every extreme that they name: `node_ids`: A token names 3 different groups; at most 13 tokens of one device name one group, and some device reaches 13 in every draw. `expert_pick`: A token names 6 different picks; pick p selects local expert p % 3 of the token's group choice p // 3.
All inputs are finite; a program needn't handle non-finite values.
Results may differ from the reference program's by a relative error of at most 0.0085.
Values may be sent and summed in bfloat16 or wider, within the bound.
A program may use at most 256 MiB of HBM per device.

```python
import math
import jax
import jax.numpy as jnp
import numpy as np
from jax import lax

D = 5120
FF = 1536
TOP = 6
TOP_NODES = 3
EXP_NODE = 3
TOK_DEV = 64
EXPERTS = 48
CAP = 13
TOKENS = 8192
N_NODE = 16
N_DEV = 8


def level_of(rng, extent, pieces, least, largest):
    def one(axis_at, shards_of):
        steps = jax.random.uniform(jax.random.fold_in(jax.random.fold_in(rng, 6), axis_at), (shards_of,), jnp.float32, least / len(pieces), largest / len(pieces))
        return jnp.repeat(jnp.exp(steps), extent[axis_at] // shards_of).reshape((-1,) + (1,) * (len(extent) - axis_at - 1))

    gain = one(*pieces[0])
    for cut in pieces[1:]:
        gain = gain * one(*cut)
    return gain


def different_ones(own_key, rows, count, top, lift):
    order = jax.random.permutation(jax.random.fold_in(own_key, 1), count)
    pull = order
    for power in range(3):
        pull = pull * pull // count
    pull = pull * lift // count
    lots = jax.random.randint(jax.random.fold_in(own_key, 2), (rows, count), 0, 4096) + pull
    fixed_rows = jax.random.permutation(jax.random.fold_in(own_key, 3), rows)[jnp.arange(count) % rows]
    lots = jnp.where(jnp.arange(rows)[:, None] == fixed_rows[None, :], 1 << 14, lots)
    merit = lots * count + jnp.arange(count)
    return lax.top_k(merit.astype(jnp.int32), top)[1].astype(jnp.int32)


def deal_out(rng, own, number, rows, count, top, bound, lean):
    sequence = jax.random.permutation(rng, count)
    packed, common = portions_of(count, rows * top, bound, lean, True), portions_of(count, rows * top, bound, lean, False)
    places = jnp.arange(count)

    def named(lengths, offset_by):
        used = int((lengths > 0).sum())
        fixed = max(1, used // 4)
        passed = fixed + (places - fixed + offset_by * (used - fixed)) % max(1, count - fixed)
        return jnp.zeros((count,), jnp.int32).at[sequence[jnp.where(places < fixed, places, passed)]].set(jnp.asarray(lengths, jnp.int32))

    lengths = jnp.where(number % 4 == 0, named(packed, number // 4), named(common, number - number // 4 - 1))
    mixed = jax.random.permutation(jax.random.fold_in(own, 3), count)
    donor, receiver = mixed[0:count // 2 * 2:2], mixed[1:count // 2 * 2:2]
    slack = jnp.minimum(lengths[donor] - 1, bound - lengths[receiver]) // 2
    slack = jnp.where((donor == sequence[0]) | (receiver == sequence[0]) | (lengths[receiver] == 0), 0, jnp.maximum(slack, 0))
    passed = jax.random.randint(jax.random.fold_in(own, 4), (count // 2,), 0, 1 << 20) % (slack + 1)
    lengths = lengths.at[donor].add(-passed).at[receiver].add(passed)
    members = jnp.searchsorted(jnp.cumsum(lengths), jnp.arange(rows * top), side="right").astype(jnp.int32)
    table = members.reshape(top, rows).T
    table = table[jax.random.permutation(jax.random.fold_in(own, 1), rows)]
    offset_by = jax.random.randint(jax.random.fold_in(own, 2), (rows, 1), 0, top)
    return jnp.take_along_axis(table, (jnp.arange(top)[None, :] + offset_by) % top, axis=1)


def portions_of(count, total, bound, slope, full):
    loads = [(1 << 20) // math.isqrt(grade ** slope) + 1 for grade in range(1, count + 1)]
    largest = bound if full else min(bound, max(-(-total // count), total * loads[0] // sum(loads)))
    least = 1 if total - largest >= count - 1 else 0
    given, surplus = [largest] + [least] * (count - 1), total - largest - least * (count - 1)
    while surplus > 0:
        free = [i for i in range(1, count) if given[i] < largest] or [i for i in range(1, count) if given[i] < bound]
        whole, left = sum([loads[i] for i in free]), surplus
        for i in free:
            extra = min(bound - given[i], max(1, left * loads[i] // whole), surplus)
            given[i] = given[i] + extra
            surplus = surplus - extra
    return np.array(given)


def noise(key, dims, spread, bound, cuts=(), kind=jnp.bfloat16):
    drawn = jax.random.normal(key, dims, jnp.float32) * spread
    if len(cuts) > 0:
        drawn = level_of(key, dims, cuts, -0.22, 0.18) * drawn
    return jnp.clip(drawn, min=-bound, max=bound).astype(kind)


def setup_inputs(seed: int = 0) -> dict:
    streams_of = jax.random.split(jax.random.key(seed), 8)
    tokens = noise(streams_of[0], (TOKENS, D), 1.0, 6.0, ((0, 128),))
    node_ids_keys = jax.random.split(jax.random.fold_in(streams_of[1], 1), TOKENS // TOK_DEV)
    node_ids_turns = jax.random.permutation(jax.random.fold_in(streams_of[1], 3), TOKENS // TOK_DEV)
    node_ids = jax.vmap(lambda own, number: deal_out(jax.random.fold_in(streams_of[1], 2), own, number, TOK_DEV, N_NODE, TOP_NODES, CAP, 2))(node_ids_keys, node_ids_turns).reshape((TOKENS, TOP_NODES))
    expert_pick = different_ones(streams_of[2], TOKENS, TOP_NODES * EXP_NODE, TOP, 0)
    gate_share = jnp.clip(jnp.exp(math.log(1.0) - 2.306499 * jax.random.uniform(streams_of[3], (TOKENS, TOP), jnp.float32) ** level_of(streams_of[3], (TOKENS, TOP), ((0, 128),), -0.2, 0.2)), 0.099609375, 1.0).astype(jnp.bfloat16)
    gate_proj = noise(streams_of[4], (EXPERTS, FF, D), D ** -0.5, 0.078125, ((0, 16), (1, 8)))
    up_proj = noise(streams_of[5], (EXPERTS, FF, D), D ** -0.5, 0.078125, ((0, 16), (1, 8)))
    down_proj = noise(streams_of[6], (EXPERTS, FF, D), FF ** -0.5, 0.15625, ((0, 16), (1, 8)))
    return {"tokens": tokens, "node_ids": node_ids, "expert_pick": expert_pick, "gate_share": gate_share, "gate_proj": gate_proj, "up_proj": up_proj, "down_proj": down_proj}


def reference(tokens, node_ids, expert_pick, gate_share, gate_proj, up_proj, down_proj):
    token_count = tokens.shape[0]
    capacity = CAP * N_NODE * N_DEV
    candidates = TOP_NODES * EXP_NODE
    slice_width = FF // N_DEV
    picked = (expert_pick[:, :, None] == jnp.arange(candidates, dtype=jnp.int32)[None, None, :]).astype(jnp.float32)
    shares = jnp.einsum('tj,tjq->tq', gate_share.astype(jnp.float32), picked, precision=lax.Precision.HIGHEST)
    shares = shares.reshape(token_count, TOP_NODES, EXP_NODE)
    contract = (((1,), (1,)), ((), ()))

    def per_node(total, node_index):
        hit_mask = (node_ids == node_index).astype(jnp.int32)
        chosen = jnp.sum(hit_mask, axis=1) > 0
        positions = jnp.nonzero(chosen, size=capacity, fill_value=0)[0].astype(jnp.int32)
        is_valid = (jnp.arange(capacity, dtype=jnp.int32) < jnp.sum(chosen.astype(jnp.int32))).astype(jnp.float32)
        node_shares = jnp.einsum('tk,tke->te', hit_mask.astype(jnp.float32), shares, precision=lax.Precision.HIGHEST)
        node_shares = node_shares[positions] * is_valid[:, None]
        tok_rows = tokens[positions]
        accumulated = jnp.zeros((capacity, N_DEV, D), jnp.float32)
        for expert_local in range(EXP_NODE):
            expert = (node_index * EXP_NODE + expert_local).astype(jnp.int32)
            w_gate = lax.dynamic_index_in_dim(gate_proj, expert, 0, keepdims=False)
            w_up = lax.dynamic_index_in_dim(up_proj, expert, 0, keepdims=False)
            w_down = lax.dynamic_index_in_dim(down_proj, expert, 0, keepdims=False)
            gate_val = lax.dot_general(tok_rows, w_gate, contract, preferred_element_type=jnp.float32)
            up_val = lax.dot_general(tok_rows, w_up, contract, preferred_element_type=jnp.float32)
            hidden = (jax.nn.silu(gate_val) * up_val).astype(jnp.bfloat16)
            grouped = jnp.einsum('rgf,gfd->rgd', hidden.reshape(capacity, N_DEV, slice_width).astype(jnp.float32),
                                 w_down.reshape(N_DEV, slice_width, D).astype(jnp.float32),
                                 precision=lax.Precision.HIGHEST)
            accumulated = accumulated + node_shares[:, expert_local, None, None] * grouped
        partial_value = lax.optimization_barrier(accumulated.astype(jnp.bfloat16)).astype(jnp.float32)
        contrib = jnp.sum(partial_value, axis=1) * is_valid[:, None]
        return total.at[positions].add(contrib), None

    total, _ = lax.scan(per_node, jnp.zeros((token_count, D), jnp.float32), jnp.arange(N_NODE, dtype=jnp.int32))
    return total.astype(jnp.bfloat16)
```

```python
import functools

import jax
import jax.numpy as jnp
from jax import lax
from jax.experimental import pallas as pl
from jax.experimental.pallas import tpu as pltpu
from jax.sharding import PartitionSpec as P

MESH = pl.DeviceIdType.MESH
BF = jnp.bfloat16
F32 = jnp.float32

CAP = 13
PAD = 16
OFFS = (
    (0, 0), (0, 1), (1, 0), (3, 3),
    (3, 1), (0, 2), (2, 0), (1, 2), (2, 1), (3, 2), (2, 3), (2, 2),
    (1, 3), (1, 1), (3, 0), (0, 3),
)
N_OFF = len(OFFS)
ROWS = N_OFF * CAP
TILES = (3, 4, 3, 3)
OWN, LEFT, RIGHT, OPP = 0, 1, 2, 3


def kernel(
    tok_ref, ids_ref, pick_ref, share_ref, wg_hbm, wu_hbm, wd_hbm, out_ref,
    wg, wu, wd, xbuf, prbuf, rabuf, rbbuf, flbuf, frbuf, send, land, ret, hid, gp, sel,
    w_sem, ds_sem, dr_sem, gs_sem, gr_sem, as_sem, ar_sem, rs_sem, rr_sem, bs_sem, br_sem,
):
    toks, width = tok_ref.shape
    half = width // 2
    experts, units = wg.shape[0], wg.shape[1]
    chunks = len(TILES)
    bounds = [0]
    for t in TILES:
        bounds.append(bounds[-1] + t * PAD)
    step = min(512, half)
    slots_all = N_OFF * PAD

    me_n = lax.axis_index("node")
    me_d = lax.axis_index("dev")
    z, y = me_n // 4, me_n % 4
    x, c = me_d // 2, me_d % 2

    def node_at(dz, dy):
        return ((z + dz) % 4) * 4 + (y + dy) % 4

    def dev_at(dx, dc):
        return ((x + dx) % 4) * 2 + (c + dc) % 2

    to_right, to_left, to_core = dev_at(1, 0), dev_at(3, 0), dev_at(0, 1)

    loads = []
    for i, (src, dst) in enumerate(((wg_hbm, wg), (wu_hbm, wu), (wd_hbm, wd))):
        load = pltpu.make_async_copy(src, dst, w_sem.at[i])
        load.start()
        loads.append(load)

    barrier = pltpu.get_barrier_semaphore()
    peers = [(node_at(dz, dy), me_d) for dz, dy in OFFS[1:]]
    peers += [(me_n, dev_at(dx, dc)) for dx in range(4) for dc in range(2) if (dx, dc) != (0, 0)]
    for peer in peers:
        pl.semaphore_signal(barrier, inc=1, device_id=peer, device_id_type=MESH)

    def remote(src, dst, s_sem, r_sem, device):
        return pltpu.make_async_remote_copy(
            src_ref=src, dst_ref=dst, send_sem=s_sem, recv_sem=r_sem,
            device_id=device, device_id_type=MESH,
        )

    col = lax.broadcasted_iota(jnp.int32, (toks, slots_all), 1)
    block, slot = col // PAD, col % PAD
    dest = jnp.zeros((toks, slots_all), jnp.int32)
    for r, (dz, dy) in enumerate(OFFS):
        dest = jnp.where(block == r, node_at(dz, dy), dest)
    ids = ids_ref[...]
    choice = [(ids[:, k : k + 1] == dest).astype(F32) for k in range(ids.shape[1])]
    chosen = choice[0] + choice[1] + choice[2]
    earlier = (
        lax.broadcasted_iota(jnp.int32, (toks, toks), 0)
        > lax.broadcasted_iota(jnp.int32, (toks, toks), 1)
    ).astype(BF)
    rank = jnp.dot(earlier, chosen.astype(BF), preferred_element_type=F32)
    picked = jnp.where(rank == slot.astype(F32), chosen, 0.0)
    sel[...] = picked.astype(BF)
    sel_t = picked.T.astype(BF)
    pick, share = pick_ref[...], share_ref[...].astype(F32)
    gates = jnp.zeros((slots_all, 128), F32)
    lane = lax.broadcasted_iota(jnp.int32, (toks, 128), 1)
    for e in range(experts):
        weight = jnp.zeros((toks, slots_all), F32)
        for k in range(len(choice)):
            part = jnp.sum(jnp.where(pick == k * experts + e, share, 0.0), axis=1, keepdims=True)
            weight = weight + choice[k] * part
        weight_t = (weight * picked).T.astype(BF)
        gates = gates + jnp.dot(weight_t, (lane == e).astype(BF), preferred_element_type=F32)
    send[:, :, width:] = gates.astype(BF).reshape(N_OFF, PAD, 128)

    def fill_send(i, carry):
        cols = pl.ds(pl.multiple_of(i * step, step), step)
        rows = jnp.dot(sel_t, tok_ref[:, cols], preferred_element_type=F32)
        send[:, :, cols] = rows.astype(BF).reshape(N_OFF, PAD, step)
        return carry

    lax.fori_loop(0, width // step, fill_send, 0)

    pl.semaphore_wait(barrier, len(peers))
    dispatch = [None]
    for r in range(1, N_OFF):
        copy = remote(
            send.at[r], land.at[r], ds_sem.at[r], dr_sem.at[r], (node_at(*OFFS[r]), me_d)
        )
        copy.start()
        dispatch.append(copy)
    land[0] = send[0]

    def rows_of(k):
        return pl.ds(bounds[k], bounds[k + 1] - bounds[k])

    low, high = pl.ds(0, half), pl.ds(half, half)
    all_cols = pl.ds(0, width)

    def gather_copy(k, j, src, dst, cols, device):
        return remote(
            xbuf.at[src, rows_of(k), cols], xbuf.at[dst, rows_of(k), cols],
            as_sem.at[k, j], ar_sem.at[k, j], (me_n, device),
        )

    gather = [
        (
            gather_copy(k, 0, OWN, LEFT, all_cols, to_right),
            gather_copy(k, 1, OWN, RIGHT, all_cols, to_left),
            gather_copy(k, 2, LEFT, OPP, low, to_right),
            gather_copy(k, 3, RIGHT, OPP, high, to_left),
            gather_copy(k, 4, OWN, 4 + OWN, all_cols, to_core),
            gather_copy(k, 5, LEFT, 4 + LEFT, all_cols, to_core),
            gather_copy(k, 6, RIGHT, 4 + RIGHT, all_cols, to_core),
            gather_copy(k, 7, OPP, 4 + OPP, all_cols, to_core),
        )
        for k in range(chunks)
    ]

    def spread(rows, row0, slots, slot0):
        at = lax.broadcasted_iota(jnp.int32, (rows, slots), 0) + row0
        frm = lax.broadcasted_iota(jnp.int32, (rows, slots), 1) + slot0
        same = at == CAP * (frm // PAD) + frm % PAD
        return (same & (frm % PAD < CAP)).astype(BF)

    arrived = [0]

    def deliver(k):
        lo, hi = bounds[k], bounds[k + 1]
        first, last = lo // CAP, min(N_OFF, (hi - 1) // CAP + 1)
        while arrived[0] < last - 1:
            arrived[0] += 1
            dispatch[arrived[0]].wait_recv()
        pack = spread(hi - lo, lo, (last - first) * PAD, first * PAD)

        def body(i, carry):
            cols = pl.ds(pl.multiple_of(i * step, step), step)
            got = land[first:last, :, cols].reshape((last - first) * PAD, step)
            xbuf[OWN, lo:hi, cols] = jnp.dot(pack, got, preferred_element_type=F32).astype(BF)
            return carry

        lax.fori_loop(0, width // step, body, 0)
        for j in (0, 1, 4):
            gather[k][j].start()

    def relay(k):
        gather[k][0].wait_recv()
        gather[k][2].start()
        gather[k][5].start()
        gather[k][1].wait_recv()
        gather[k][3].start()
        gather[k][6].start()

    def relay_opp(k):
        gather[k][2].wait_recv()
        gather[k][3].wait_recv()
        gather[k][7].start()

    gate_copies = []

    def share_gates():
        pack = spread(ROWS, 0, slots_all, 0)
        got = land[:, :, width:].reshape(slots_all, 128)
        flat = jnp.dot(pack, got, preferred_element_type=F32).astype(BF)
        packed = jnp.zeros((PAD, 128), F32)
        e_at = lax.broadcasted_iota(jnp.int32, (128, 128), 0)
        l_at = lax.broadcasted_iota(jnp.int32, (128, 128), 1)
        for t in range(ROWS // PAD):
            move = ((e_at < experts) & (l_at == experts * t + e_at)).astype(BF)
            packed = packed + jnp.dot(
                flat[t * PAD : (t + 1) * PAD], move, preferred_element_type=F32
            )
        gp[0] = packed.astype(BF)
        n = 0
        for dx, there in ((0, OWN), (1, LEFT), (3, RIGHT), (2, OPP)):
            for dc in (0, 1):
                if (dx, dc) == (0, 0):
                    continue
                copy = remote(
                    gp.at[0], gp.at[4 * dc + there], gs_sem.at[n], gr_sem.at[n],
                    (me_n, dev_at(dx, dc)),
                )
                copy.start()
                gate_copies.append(copy)
                n += 1

    def hidden(k):
        lo, hi = bounds[k], bounds[k + 1]
        m = 8 * (hi - lo)
        for j in (4, 5, 6, 7):
            gather[k][j].wait_recv()
        contract = (((1,), (1,)), ((), ()))
        columns = []
        for e in range(experts):
            pieces = []
            for s in range(8):
                for t in range(lo // PAD, hi // PAD):
                    at = experts * t + e
                    pieces.append(gp[s, :, at : at + 1].astype(F32))
            columns.append(jnp.concatenate(pieces, axis=0))
        for e in range(experts):
            rows = xbuf[:, lo:hi, :].reshape(m, width)
            gate_val = lax.dot_general(rows, wg[e], contract, preferred_element_type=F32)
            up_val = lax.dot_general(rows, wu[e], contract, preferred_element_type=F32)
            act = gate_val / (1.0 + jnp.exp(-gate_val)) * up_val
            hid[e, 0:m, :] = (act * columns[e]).astype(BF)

    def reduce_copy(k, j, src, dst, cols, device, n=None):
        return remote(
            src.at[rows_of(k), cols], dst.at[rows_of(k), cols],
            rs_sem.at[k, j], rr_sem.at[k, j], (me_n, device),
        )

    reduce = [
        (
            remote(
                xbuf.at[4:8, rows_of(k), low], prbuf.at[:, rows_of(k), low],
                rs_sem.at[k, 0], rr_sem.at[k, 0], (me_n, to_core),
            ),
            remote(
                xbuf.at[4:8, rows_of(k), high], prbuf.at[:, rows_of(k), high],
                rs_sem.at[k, 1], rr_sem.at[k, 1], (me_n, to_core),
            ),
            reduce_copy(k, 2, xbuf.at[OPP, :, low], rabuf, low, to_right),
            reduce_copy(k, 3, xbuf.at[OPP, :, high], rbbuf, low, to_left),
            reduce_copy(k, 4, xbuf.at[RIGHT], flbuf, high, to_right),
            reduce_copy(k, 5, xbuf.at[LEFT], frbuf, low, to_left),
            reduce_copy(k, 6, xbuf.at[RIGHT], flbuf, low, to_right),
            reduce_copy(k, 7, xbuf.at[LEFT], frbuf, high, to_left),
        )
        for k in range(chunks)
    ]

    def project(k):
        lo, hi = bounds[k], bounds[k + 1]
        m = 8 * (hi - lo)
        for j in range(8):
            gather[k][j].wait_send()

        def body(i, carry):
            cols = pl.ds(pl.multiple_of(i * step, step), step)
            total = jnp.dot(hid[0, 0:m, :], wd[0, :, cols], preferred_element_type=F32)
            for e in range(1, experts):
                total += jnp.dot(hid[e, 0:m, :], wd[e, :, cols], preferred_element_type=F32)
            xbuf[:, lo:hi, cols] = total.astype(BF).reshape(8, hi - lo, step)
            return carry

        lax.fori_loop(0, half // step, body, 0)
        reduce[k][0].start()
        lax.fori_loop(half // step, width // step, body, 0)
        reduce[k][1].start()

    def add_up(k, place, start, others):
        lo, hi = bounds[k], bounds[k + 1]

        def body(i, carry):
            at = pl.multiple_of(i * step, step)
            cols = pl.ds(start + at, step)
            total = xbuf[place, lo:hi, cols].astype(F32)
            for other, shift in others:
                total += other[lo:hi, pl.ds(at + shift, step)].astype(F32)
            xbuf[place, lo:hi, cols] = total.astype(BF)
            return carry

        lax.fori_loop(0, half // step, body, 0)

    def pass_on(k):
        reduce[k][0].wait_recv()
        add_up(k, OPP, 0, ((prbuf.at[OPP], 0),))
        reduce[k][2].start()
        reduce[k][1].wait_recv()
        add_up(k, OPP, half, ((prbuf.at[OPP], half),))
        reduce[k][3].start()
        add_up(k, RIGHT, half, ((prbuf.at[RIGHT], half),))
        reduce[k][4].start()
        add_up(k, LEFT, 0, ((prbuf.at[LEFT], 0),))
        reduce[k][5].start()

    def pass_home(k):
        reduce[k][2].wait_recv()
        add_up(k, RIGHT, 0, ((prbuf.at[RIGHT], 0), (rabuf, 0)))
        reduce[k][6].start()
        reduce[k][3].wait_recv()
        add_up(k, LEFT, half, ((prbuf.at[LEFT], half), (rbbuf, 0)))
        reduce[k][7].start()

    returns = [None]
    returned = [0]

    def give_back(k):
        lo, hi = bounds[k], bounds[k + 1]
        for j in (4, 5, 6, 7):
            reduce[k][j].wait_recv()
        for start in (0, half):
            add_up(k, OWN, start, ((prbuf.at[OWN], start), (flbuf, start), (frbuf, start)))
        first, last = returned[0], hi // CAP
        returned[0] = last
        row0 = first * CAP // PAD * PAD
        unpack = (
            lax.broadcasted_iota(jnp.int32, ((last - first) * PAD, hi - row0), 1) + row0
        )
        frm = lax.broadcasted_iota(jnp.int32, ((last - first) * PAD, hi - row0), 0) + first * PAD
        unpack = ((unpack == CAP * (frm // PAD) + frm % PAD) & (frm % PAD < CAP)).astype(BF)
        own = 1 if first == 0 else 0

        def body(i, carry):
            cols = pl.ds(pl.multiple_of(i * step, step), step)
            back = jnp.dot(unpack, xbuf[OWN, row0:hi, cols], preferred_element_type=F32)
            back = back.astype(BF).reshape(last - first, PAD, step)
            if own:
                ret[0, :, cols] = back[0]
            send[first + own : last, :, cols] = back[own:]
            return carry

        lax.fori_loop(0, width // step, body, 0)
        for r in range(first + own, last):
            dz, dy = OFFS[r]
            copy = remote(
                send.at[r, :, all_cols], ret.at[r], bs_sem.at[r], br_sem.at[r],
                (node_at(-dz, -dy), me_d),
            )
            copy.start()
            returns.append(copy)

    deliver(0)
    deliver(1)
    relay(0)
    deliver(2)
    relay(1)
    relay_opp(0)
    deliver(3)
    share_gates()
    relay(2)
    relay_opp(1)
    for load in loads:
        load.wait()
    for copy in gate_copies:
        copy.wait_recv()
    hidden(0)
    project(0)
    relay(3)
    relay_opp(2)
    hidden(1)
    pass_on(0)
    project(1)
    relay_opp(3)
    pass_home(0)
    hidden(2)
    pass_on(1)
    project(2)
    pass_home(1)
    hidden(3)
    pass_on(2)
    project(3)
    for r in range(1, N_OFF):
        dispatch[r].wait_send()
    pass_on(3)
    give_back(0)
    pass_home(2)
    give_back(1)
    pass_home(3)
    give_back(2)
    give_back(3)

    for r in range(1, N_OFF):
        returns[r].wait_recv()

    def combine(i, carry):
        cols = pl.ds(pl.multiple_of(i * step, step), step)
        got = ret[:, :, cols].reshape(slots_all, step)
        out_ref[:, cols] = jnp.dot(sel[...], got, preferred_element_type=F32).astype(BF)
        return carry

    lax.fori_loop(0, width // step, combine, 0)

    for copy in gate_copies:
        copy.wait_send()
    for k in range(chunks):
        for copy in reduce[k]:
            copy.wait_send()
    for r in range(1, N_OFF):
        returns[r].wait_send()


def shards(tokens, node_ids, expert_pick, gate_share, gate_proj, up_proj, down_proj):
    toks, width = tokens.shape
    experts, units, _ = gate_proj.shape
    half = width // 2
    chunks = len(TILES)
    vmem = pl.BlockSpec(memory_space=pltpu.VMEM)
    hbm = pl.BlockSpec(memory_space=pl.ANY)
    dma = pltpu.SemaphoreType.DMA
    weights = pltpu.VMEM((experts, units, width), BF)
    return pl.pallas_call(
        kernel,
        out_shape=jax.ShapeDtypeStruct((toks, width), BF),
        in_specs=[vmem] * 4 + [hbm] * 3,
        out_specs=vmem,
        scratch_shapes=[
            weights,
            weights,
            weights,
            pltpu.VMEM((8, ROWS, width), BF),
            pltpu.VMEM((4, ROWS, width), BF),
            pltpu.VMEM((ROWS, half), BF),
            pltpu.VMEM((ROWS, half), BF),
            pltpu.VMEM((ROWS, width), BF),
            pltpu.VMEM((ROWS, width), BF),
            pltpu.VMEM((N_OFF, PAD, width + 128), BF),
            pltpu.VMEM((N_OFF, PAD, width + 128), BF),
            pltpu.VMEM((N_OFF, PAD, width), BF),
            pltpu.VMEM((experts, 8 * PAD * max(TILES), units), BF),
            pltpu.VMEM((8, PAD, 128), BF),
            pltpu.VMEM((toks, N_OFF * PAD), BF),
            dma((3,)),
            dma((N_OFF,)),
            dma((N_OFF,)),
            dma((7,)),
            dma((7,)),
            dma((chunks, 8)),
            dma((chunks, 8)),
            dma((chunks, 8)),
            dma((chunks, 8)),
            dma((N_OFF,)),
            dma((N_OFF,)),
        ],
        compiler_params=pltpu.CompilerParams(
            collective_id=0, has_side_effects=True, vmem_limit_bytes=67043328
        ),
    )(tokens, node_ids, expert_pick, gate_share, gate_proj, up_proj, down_proj)


def solution(mesh):
    return jax.shard_map(
        shards,
        mesh=mesh,
        in_specs=(
            P(("node", "dev"), None),
            P(("node", "dev"), None),
            P(("node", "dev"), None),
            P(("node", "dev"), None),
            P("node", "dev", None),
            P("node", "dev", None),
            P("node", "dev", None),
        ),
        out_specs=P(("node", "dev"), None),
        check_vma=False,
    )
```

```python
import functools

import jax
import jax.numpy as jnp
from jax import lax
from jax.experimental import pallas as pl
from jax.experimental.pallas import tpu as pltpu
from jax.sharding import PartitionSpec as P

MESH = pl.DeviceIdType.MESH
BF = jnp.bfloat16
F32 = jnp.float32

CAP = 13
PAD = 16
OFFS = (
    (0, 0), (0, 1), (1, 0), (3, 3),
    (2, 2), (1, 2), (2, 1), (0, 2), (2, 0),
    (3, 2), (2, 3), (3, 1), (1, 3),
    (1, 1), (3, 0), (0, 3),
)
N_OFF = len(OFFS)
WAVES = (1, 4, 9, N_OFF)
ROWS = N_OFF * CAP
TILES = (3, 4, 4, 2)
OWN, LEFT, RIGHT, OPP = 0, 1, 2, 3


def kernel(
    tok_ref, ids_ref, pick_ref, share_ref, wg_hbm, wu_hbm, wd_hbm, out_ref,
    wg, wu, wd, xbuf, prbuf, rabuf, rbbuf, flbuf, frbuf, send, land, ret, hid, gp, sel, total,
    o_sem, w_sem, ds_sem, dr_sem, gs_sem, gr_sem, as_sem, ar_sem, rs_sem, rr_sem, bs_sem, br_sem,
):
    toks, width = tok_ref.shape
    half = width // 2
    experts, units = wg.shape[0], wg.shape[1]
    chunks = len(TILES)
    bounds = [0]
    for t in TILES:
        bounds.append(bounds[-1] + t * PAD)
    step = min(512, half)
    slots_all = N_OFF * PAD

    me_n = lax.axis_index("node")
    me_d = lax.axis_index("dev")
    z, y = me_n // 4, me_n % 4
    x, c = me_d // 2, me_d % 2

    def node_at(dz, dy):
        return ((z + dz) % 4) * 4 + (y + dy) % 4

    def dev_at(dx, dc):
        return ((x + dx) % 4) * 2 + (c + dc) % 2

    to_right, to_left, to_core = dev_at(1, 0), dev_at(3, 0), dev_at(0, 1)

    loads = []
    for i, (src, dst) in enumerate(((wg_hbm, wg), (wu_hbm, wu), (wd_hbm, wd))):
        load = pltpu.make_async_copy(src, dst, w_sem.at[i])
        load.start()
        loads.append(load)

    barrier = pltpu.get_barrier_semaphore()
    peers = [(node_at(dz, dy), me_d) for dz, dy in OFFS[1:]]
    peers += [(me_n, dev_at(dx, dc)) for dx in range(4) for dc in range(2) if (dx, dc) != (0, 0)]
    for peer in peers:
        pl.semaphore_signal(barrier, inc=1, device_id=peer, device_id_type=MESH)

    def remote(src, dst, s_sem, r_sem, device):
        return pltpu.make_async_remote_copy(
            src_ref=src, dst_ref=dst, send_sem=s_sem, recv_sem=r_sem,
            device_id=device, device_id_type=MESH,
        )

    row = lax.broadcasted_iota(jnp.int32, (slots_all, toks), 0)
    block, slot = row // PAD, row % PAD
    dest = jnp.zeros((slots_all, toks), jnp.int32)
    for r, (dz, dy) in enumerate(OFFS):
        dest = jnp.where(block == r, node_at(dz, dy), dest)
    ids = ids_ref[...]
    choice = [(ids[k : k + 1, :] == dest).astype(F32) for k in range(ids.shape[0])]
    chosen = choice[0] + choice[1] + choice[2]
    earlier = (
        lax.broadcasted_iota(jnp.int32, (toks, toks), 0)
        < lax.broadcasted_iota(jnp.int32, (toks, toks), 1)
    ).astype(BF)
    rank = jnp.dot(chosen.astype(BF), earlier, preferred_element_type=F32)
    picked = jnp.where(rank == slot.astype(F32), chosen, 0.0)
    sel_t = picked.astype(BF)
    pick, share = pick_ref[...], share_ref[...].astype(F32)
    gates = jnp.zeros((slots_all, 128), F32)
    lane = lax.broadcasted_iota(jnp.int32, (toks, 128), 1)
    for e in range(experts):
        weight = jnp.zeros((slots_all, toks), F32)
        for k in range(len(choice)):
            part = jnp.sum(jnp.where(pick == k * experts + e, share, 0.0), axis=0, keepdims=True)
            weight = weight + choice[k] * part
        weight = (weight * picked).astype(BF)
        gates = gates + jnp.dot(weight, (lane == e).astype(BF), preferred_element_type=F32)
    send[:, :, width:] = gates.astype(BF).reshape(N_OFF, PAD, 128)

    def fill_send(i, carry):
        cols = pl.ds(pl.multiple_of(i * step, step), step)
        rows = jnp.dot(sel_t, tok_ref[:, cols], preferred_element_type=F32)
        send[:, :, cols] = rows.astype(BF).reshape(N_OFF, PAD, step)
        return carry

    lax.fori_loop(0, width // step, fill_send, 0)

    pl.semaphore_wait(barrier, len(peers))
    dispatch = [None]
    for r in range(1, N_OFF):
        copy = remote(
            send.at[r], land.at[r], ds_sem.at[r], dr_sem.at[r], (node_at(*OFFS[r]), me_d)
        )
        dispatch.append(copy)
    for r in range(WAVES[0], WAVES[1]):
        dispatch[r].start()
    land[0] = send[0]
    sel[...] = picked.T.astype(BF)

    def rows_of(k):
        return pl.ds(bounds[k], bounds[k + 1] - bounds[k])

    low, high = pl.ds(0, half), pl.ds(half, half)
    all_cols = pl.ds(0, width)

    def gather_copy(k, j, src, dst, cols, device):
        return remote(
            xbuf.at[src, rows_of(k), cols], xbuf.at[dst, rows_of(k), cols],
            as_sem.at[k, j], ar_sem.at[k, j], (me_n, device),
        )

    gather = [
        (
            gather_copy(k, 0, OWN, LEFT, all_cols, to_right),
            gather_copy(k, 1, OWN, RIGHT, all_cols, to_left),
            gather_copy(k, 2, LEFT, OPP, low, to_right),
            gather_copy(k, 3, RIGHT, OPP, high, to_left),
            gather_copy(k, 4, OWN, 4 + OWN, all_cols, to_core),
            gather_copy(k, 5, LEFT, 4 + LEFT, all_cols, to_core),
            gather_copy(k, 6, RIGHT, 4 + RIGHT, all_cols, to_core),
            gather_copy(k, 7, OPP, 4 + OPP, all_cols, to_core),
        )
        for k in range(chunks)
    ]

    def spread(rows, row0, slots, slot0):
        at = lax.broadcasted_iota(jnp.int32, (rows, slots), 0) + row0
        frm = lax.broadcasted_iota(jnp.int32, (rows, slots), 1) + slot0
        same = at == CAP * (frm // PAD) + frm % PAD
        return (same & (frm % PAD < CAP)).astype(BF)

    arrived = [0]
    gate_copies = []

    def share_gates(k, pack, got):
        flat = jnp.dot(pack, got, preferred_element_type=F32).astype(BF)
        packed = jnp.zeros((PAD, 128), F32)
        e_at = lax.broadcasted_iota(jnp.int32, (128, 128), 0)
        l_at = lax.broadcasted_iota(jnp.int32, (128, 128), 1)
        for t in range(TILES[k]):
            move = ((e_at < experts) & (l_at == experts * t + e_at)).astype(BF)
            packed = packed + jnp.dot(
                flat[t * PAD : (t + 1) * PAD], move, preferred_element_type=F32
            )
        gp[k, 0] = packed.astype(BF)
        copies = []
        for dx, there in ((0, OWN), (1, LEFT), (3, RIGHT), (2, OPP)):
            for dc in (0, 1):
                if (dx, dc) == (0, 0):
                    continue
                n = len(copies)
                copy = remote(
                    gp.at[k, 0], gp.at[k, 4 * dc + there], gs_sem.at[k, n], gr_sem.at[k, n],
                    (me_n, dev_at(dx, dc)),
                )
                copy.start()
                copies.append(copy)
        gate_copies.append(copies)

    def deliver(k):
        lo, hi = bounds[k], bounds[k + 1]
        first, last = lo // CAP, min(N_OFF, (hi - 1) // CAP + 1)
        while arrived[0] < last - 1:
            arrived[0] += 1
            dispatch[arrived[0]].wait_recv()
        if k + 2 < len(WAVES):
            for r in range(WAVES[k + 1], WAVES[k + 2]):
                dispatch[r].start()
        pack = spread(hi - lo, lo, (last - first) * PAD, first * PAD)
        share_gates(k, pack, land[first:last, :, width:].reshape((last - first) * PAD, 128))

        def body(i, carry):
            cols = pl.ds(pl.multiple_of(i * step, step), step)
            got = land[first:last, :, cols].reshape((last - first) * PAD, step)
            xbuf[OWN, lo:hi, cols] = jnp.dot(pack, got, preferred_element_type=F32).astype(BF)
            return carry

        lax.fori_loop(0, width // step, body, 0, unroll=5)
        for j in (0, 1, 4):
            gather[k][j].start()

    def relay(k):
        gather[k][0].wait_recv()
        gather[k][2].start()
        gather[k][5].start()
        gather[k][1].wait_recv()
        gather[k][3].start()
        gather[k][6].start()

    def relay_opp(k):
        gather[k][2].wait_recv()
        gather[k][3].wait_recv()
        gather[k][7].start()

    def hidden(k):
        lo, hi = bounds[k], bounds[k + 1]
        m = 8 * (hi - lo)
        for j in (4, 5, 6, 7):
            gather[k][j].wait_recv()
        for copy in gate_copies[k]:
            copy.wait_recv()
        contract = (((1,), (1,)), ((), ()))
        columns = []
        for e in range(experts):
            pieces = []
            for s in range(8):
                for t in range(TILES[k]):
                    at = experts * t + e
                    pieces.append(gp[k, s, :, at : at + 1].astype(F32))
            columns.append(jnp.concatenate(pieces, axis=0))
        for e in range(experts):
            rows = xbuf[:, lo:hi, :].reshape(m, width)
            gate_val = lax.dot_general(rows, wg[e], contract, preferred_element_type=F32)
            up_val = lax.dot_general(rows, wu[e], contract, preferred_element_type=F32)
            act = gate_val / (1.0 + jnp.exp(-gate_val)) * up_val
            hid[e, 0:m, :] = (act * columns[e]).astype(BF)

    def reduce_copy(k, j, src, dst, cols, device, n=None):
        return remote(
            src.at[rows_of(k), cols], dst.at[rows_of(k), cols],
            rs_sem.at[k, j], rr_sem.at[k, j], (me_n, device),
        )

    reduce = [
        (
            remote(
                xbuf.at[4:8, rows_of(k), low], prbuf.at[:, rows_of(k), low],
                rs_sem.at[k, 0], rr_sem.at[k, 0], (me_n, to_core),
            ),
            remote(
                xbuf.at[4:8, rows_of(k), high], prbuf.at[:, rows_of(k), high],
                rs_sem.at[k, 1], rr_sem.at[k, 1], (me_n, to_core),
            ),
            reduce_copy(k, 2, xbuf.at[OPP, :, low], rabuf, low, to_right),
            reduce_copy(k, 3, xbuf.at[OPP, :, high], rbbuf, low, to_left),
            reduce_copy(k, 4, xbuf.at[RIGHT], flbuf, high, to_right),
            reduce_copy(k, 5, xbuf.at[LEFT], frbuf, low, to_left),
            reduce_copy(k, 6, xbuf.at[RIGHT], flbuf, low, to_right),
            reduce_copy(k, 7, xbuf.at[LEFT], frbuf, high, to_left),
        )
        for k in range(chunks)
    ]

    def project(k):
        lo, hi = bounds[k], bounds[k + 1]
        m = 8 * (hi - lo)
        for j in range(8):
            gather[k][j].wait_send()

        def body(i, carry):
            cols = pl.ds(pl.multiple_of(i * step, step), step)
            total = jnp.dot(hid[0, 0:m, :], wd[0, :, cols], preferred_element_type=F32)
            for e in range(1, experts):
                total += jnp.dot(hid[e, 0:m, :], wd[e, :, cols], preferred_element_type=F32)
            xbuf[:, lo:hi, cols] = total.astype(BF).reshape(8, hi - lo, step)
            return carry

        lax.fori_loop(0, half // step, body, 0)
        reduce[k][0].start()
        lax.fori_loop(half // step, width // step, body, 0)
        reduce[k][1].start()

    def add_up(k, place, start, others):
        lo, hi = bounds[k], bounds[k + 1]

        def body(i, carry):
            at = pl.multiple_of(i * step, step)
            cols = pl.ds(start + at, step)
            total = xbuf[place, lo:hi, cols].astype(F32)
            for other, shift in others:
                total += other[lo:hi, pl.ds(at + shift, step)].astype(F32)
            xbuf[place, lo:hi, cols] = total.astype(BF)
            return carry

        lax.fori_loop(0, half // step, body, 0)

    def pass_on(k):
        reduce[k][0].wait_recv()
        add_up(k, OPP, 0, ((prbuf.at[OPP], 0),))
        reduce[k][2].start()
        reduce[k][1].wait_recv()
        add_up(k, OPP, half, ((prbuf.at[OPP], half),))
        reduce[k][3].start()
        add_up(k, RIGHT, half, ((prbuf.at[RIGHT], half),))
        reduce[k][4].start()
        add_up(k, LEFT, 0, ((prbuf.at[LEFT], 0),))
        reduce[k][5].start()

    def pass_home(k):
        reduce[k][2].wait_recv()
        add_up(k, RIGHT, 0, ((prbuf.at[RIGHT], 0), (rabuf, 0)))
        reduce[k][6].start()
        reduce[k][3].wait_recv()
        add_up(k, LEFT, half, ((prbuf.at[LEFT], half), (rbbuf, 0)))
        reduce[k][7].start()

    returns = [None]
    returned = [0]

    def give_back(k):
        lo, hi = bounds[k], bounds[k + 1]
        for j in (4, 5, 6, 7):
            reduce[k][j].wait_recv()
        for start in (0, half):
            add_up(k, OWN, start, ((prbuf.at[OWN], start), (flbuf, start), (frbuf, start)))
        first, last = returned[0], hi // CAP
        returned[0] = last
        row0 = first * CAP // PAD * PAD
        unpack = (
            lax.broadcasted_iota(jnp.int32, ((last - first) * PAD, hi - row0), 1) + row0
        )
        frm = lax.broadcasted_iota(jnp.int32, ((last - first) * PAD, hi - row0), 0) + first * PAD
        unpack = ((unpack == CAP * (frm // PAD) + frm % PAD) & (frm % PAD < CAP)).astype(BF)
        own = 1 if first == 0 else 0

        def body(i, carry):
            cols = pl.ds(pl.multiple_of(i * step, step), step)
            back = jnp.dot(unpack, xbuf[OWN, row0:hi, cols], preferred_element_type=F32)
            back = back.astype(BF).reshape(last - first, PAD, step)
            if own:
                ret[0, :, cols] = back[0]
            send[first + own : last, :, cols] = back[own:]
            return carry

        lax.fori_loop(0, width // step, body, 0, unroll=5)
        for r in range(first + own, last):
            dz, dy = OFFS[r]
            copy = remote(
                send.at[r, :, all_cols], ret.at[r], bs_sem.at[r], br_sem.at[r],
                (node_at(-dz, -dy), me_d),
            )
            copy.start()
            returns.append(copy)

    deliver(0)
    relay(0)
    deliver(1)
    relay_opp(0)
    deliver(2)
    for load in loads:
        load.wait()
    hidden(0)
    relay(1)
    deliver(3)
    project(0)
    relay_opp(1)
    pass_on(0)
    relay(2)
    hidden(1)
    relay(3)
    relay_opp(2)
    project(1)
    pass_on(1)
    relay_opp(3)
    pass_home(0)
    hidden(2)
    project(2)
    pass_on(2)
    pass_home(1)
    hidden(3)
    project(3)
    for r in range(1, N_OFF):
        dispatch[r].wait_send()
    give_back(0)
    pass_on(3)
    pass_home(2)
    give_back(1)
    pass_home(3)
    give_back(2)
    give_back(3)

    for r in range(1, N_OFF):
        returns[r].wait_recv()
    outs = []
    parts = 2
    for p in range(parts):

        def combine(i, carry, p=p):
            cols = pl.ds(pl.multiple_of(p * (width // parts) + i * step, step), step)
            got = ret[:, :, cols].reshape(slots_all, step)
            total[:, cols] = jnp.dot(sel[...], got, preferred_element_type=F32).astype(BF)
            return carry

        lax.fori_loop(0, width // parts // step, combine, 0, unroll=5)
        cols = pl.ds(p * (width // parts), width // parts)
        copy = pltpu.make_async_copy(total.at[:, cols], out_ref.at[:, cols], o_sem.at[p])
        copy.start()
        outs.append(copy)

    for copies in gate_copies:
        for copy in copies:
            copy.wait_send()
    for k in range(chunks):
        for copy in reduce[k]:
            copy.wait_send()
    for r in range(1, N_OFF):
        returns[r].wait_send()
    for copy in outs:
        copy.wait()


def shards(tokens, node_ids, expert_pick, gate_share, gate_proj, up_proj, down_proj):
    toks, width = tokens.shape
    experts, units, _ = gate_proj.shape
    half = width // 2
    chunks = len(TILES)
    vmem = pl.BlockSpec(memory_space=pltpu.VMEM)
    hbm = pl.BlockSpec(memory_space=pl.ANY)
    dma = pltpu.SemaphoreType.DMA
    weights = pltpu.VMEM((experts, units, width), BF)
    return pl.pallas_call(
        kernel,
        out_shape=jax.ShapeDtypeStruct((toks, width), BF),
        in_specs=[vmem] * 4 + [hbm] * 3,
        out_specs=hbm,
        scratch_shapes=[
            weights,
            weights,
            weights,
            pltpu.VMEM((8, ROWS, width), BF),
            pltpu.VMEM((4, ROWS, width), BF),
            pltpu.VMEM((ROWS, half), BF),
            pltpu.VMEM((ROWS, half), BF),
            pltpu.VMEM((ROWS, width), BF),
            pltpu.VMEM((ROWS, width), BF),
            pltpu.VMEM((N_OFF, PAD, width + 128), BF),
            pltpu.VMEM((N_OFF, PAD, width + 128), BF),
            pltpu.VMEM((N_OFF, PAD, width), BF),
            pltpu.VMEM((experts, 8 * PAD * max(TILES), units), BF),
            pltpu.VMEM((chunks, 8, PAD, 128), BF),
            pltpu.VMEM((toks, N_OFF * PAD), BF),
            pltpu.VMEM((toks, width), BF),
            dma((2,)),
            dma((3,)),
            dma((N_OFF,)),
            dma((N_OFF,)),
            dma((chunks, 7)),
            dma((chunks, 7)),
            dma((chunks, 8)),
            dma((chunks, 8)),
            dma((chunks, 8)),
            dma((chunks, 8)),
            dma((N_OFF,)),
            dma((N_OFF,)),
        ],
        compiler_params=pltpu.CompilerParams(
            collective_id=0, has_side_effects=True, vmem_limit_bytes=67043328
        ),
    )(tokens, node_ids.T, expert_pick.T, gate_share.T, gate_proj, up_proj, down_proj)


def solution(mesh):
    return jax.shard_map(
        shards,
        mesh=mesh,
        in_specs=(
            P(("node", "dev"), None),
            P(("node", "dev"), None),
            P(("node", "dev"), None),
            P(("node", "dev"), None),
            P("node", "dev", None),
            P("node", "dev", None),
            P("node", "dev", None),
        ),
        out_specs=P(("node", "dev"), None),
        check_vma=False,
    )
```

```python
import functools

import jax
import jax.numpy as jnp
from jax import lax
from jax.experimental import pallas as pl
from jax.experimental.pallas import tpu as pltpu
from jax.sharding import PartitionSpec as P

MESH = pl.DeviceIdType.MESH
BF = jnp.bfloat16
F32 = jnp.float32

CAP = 13
PAD = 16
OFFS = (
    (0, 0), (0, 1), (1, 0), (3, 3),
    (2, 2), (1, 2), (2, 1), (3, 2),
    (2, 3), (0, 2), (2, 0), (3, 1), (1, 3),
    (1, 1), (3, 0), (0, 3),
)
N_OFF = len(OFFS)
WAVES = (1, 4, 9, N_OFF)
ROWS = N_OFF * CAP
TILES = (3, 4, 4, 2)
OWN, LEFT, RIGHT, OPP = 0, 1, 2, 3


def kernel(
    tok_ref, ids_ref, pick_ref, share_ref, wg_hbm, wu_hbm, wd_hbm, out_ref,
    wg, wu, wd, xbuf, prbuf, rabuf, rbbuf, flbuf, frbuf, send, land, ret, hid, gp, sel, total,
    o_sem, w_sem, ds_sem, dr_sem, gs_sem, gr_sem, as_sem, ar_sem, rs_sem, rr_sem, bs_sem, br_sem,
):
    toks, width = tok_ref.shape
    half = width // 2
    experts, units = wg.shape[0], wg.shape[1]
    chunks = len(TILES)
    bounds = [0]
    for t in TILES:
        bounds.append(bounds[-1] + t * PAD)
    step = min(512, half)
    slots_all = N_OFF * PAD

    me_n = lax.axis_index("node")
    me_d = lax.axis_index("dev")
    z, y = me_n // 4, me_n % 4
    x, c = me_d // 2, me_d % 2

    def node_at(dz, dy):
        return ((z + dz) % 4) * 4 + (y + dy) % 4

    def dev_at(dx, dc):
        return ((x + dx) % 4) * 2 + (c + dc) % 2

    to_right, to_left, to_core = dev_at(1, 0), dev_at(3, 0), dev_at(0, 1)

    loads = []
    for i, (src, dst) in enumerate(((wg_hbm, wg), (wu_hbm, wu), (wd_hbm, wd))):
        load = pltpu.make_async_copy(src, dst, w_sem.at[i])
        load.start()
        loads.append(load)

    barrier = pltpu.get_barrier_semaphore()
    peers = [(node_at(dz, dy), me_d) for dz, dy in OFFS[1:]]
    peers += [(me_n, dev_at(dx, dc)) for dx in range(4) for dc in range(2) if (dx, dc) != (0, 0)]
    for peer in peers:
        pl.semaphore_signal(barrier, inc=1, device_id=peer, device_id_type=MESH)

    def remote(src, dst, s_sem, r_sem, device):
        return pltpu.make_async_remote_copy(
            src_ref=src, dst_ref=dst, send_sem=s_sem, recv_sem=r_sem,
            device_id=device, device_id_type=MESH,
        )

    row = lax.broadcasted_iota(jnp.int32, (slots_all, toks), 0)
    block, slot = row // PAD, row % PAD
    dest = jnp.zeros((slots_all, toks), jnp.int32)
    for r, (dz, dy) in enumerate(OFFS):
        dest = jnp.where(block == r, node_at(dz, dy), dest)
    ids = ids_ref[...]
    choice = [(ids[k : k + 1, :] == dest).astype(F32) for k in range(ids.shape[0])]
    chosen = choice[0] + choice[1] + choice[2]
    earlier = (
        lax.broadcasted_iota(jnp.int32, (toks, toks), 0)
        < lax.broadcasted_iota(jnp.int32, (toks, toks), 1)
    ).astype(BF)
    rank = jnp.dot(chosen.astype(BF), earlier, preferred_element_type=F32)
    picked = jnp.where(rank == slot.astype(F32), chosen, 0.0)
    sel_t = picked.astype(BF)
    pick, share = pick_ref[...], share_ref[...].astype(F32)
    gates = jnp.zeros((slots_all, 128), F32)
    lane = lax.broadcasted_iota(jnp.int32, (toks, 128), 1)
    for e in range(experts):
        weight = jnp.zeros((slots_all, toks), F32)
        for k in range(len(choice)):
            part = jnp.sum(jnp.where(pick == k * experts + e, share, 0.0), axis=0, keepdims=True)
            weight = weight + choice[k] * part
        weight = (weight * picked).astype(BF)
        gates = gates + jnp.dot(weight, (lane == e).astype(BF), preferred_element_type=F32)
    send[:, :, width:] = gates.astype(BF).reshape(N_OFF, PAD, 128)

    def fill_send(i, carry):
        cols = pl.ds(pl.multiple_of(i * step, step), step)
        rows = jnp.dot(sel_t, tok_ref[:, cols], preferred_element_type=F32)
        send[:, :, cols] = rows.astype(BF).reshape(N_OFF, PAD, step)
        return carry

    lax.fori_loop(0, width // step, fill_send, 0)

    pl.semaphore_wait(barrier, len(peers))
    dispatch = [None]
    for r in range(1, N_OFF):
        copy = remote(
            send.at[r], land.at[r], ds_sem.at[r], dr_sem.at[r], (node_at(*OFFS[r]), me_d)
        )
        dispatch.append(copy)
    for r in range(WAVES[0], WAVES[1]):
        dispatch[r].start()
    land[0] = send[0]
    sel[...] = picked.T.astype(BF)

    def rows_of(k):
        return pl.ds(bounds[k], bounds[k + 1] - bounds[k])

    low, high = pl.ds(0, half), pl.ds(half, half)
    all_cols = pl.ds(0, width)

    def gather_copy(k, j, src, dst, cols, device):
        return remote(
            xbuf.at[src, rows_of(k), cols], xbuf.at[dst, rows_of(k), cols],
            as_sem.at[k, j], ar_sem.at[k, j], (me_n, device),
        )

    gather = [
        (
            gather_copy(k, 0, OWN, LEFT, all_cols, to_right),
            gather_copy(k, 1, OWN, RIGHT, all_cols, to_left),
            gather_copy(k, 2, LEFT, OPP, low, to_right),
            gather_copy(k, 3, RIGHT, OPP, high, to_left),
            gather_copy(k, 4, OWN, 4 + OWN, all_cols, to_core),
            gather_copy(k, 5, LEFT, 4 + LEFT, all_cols, to_core),
            gather_copy(k, 6, RIGHT, 4 + RIGHT, all_cols, to_core),
            gather_copy(k, 7, OPP, 4 + OPP, all_cols, to_core),
        )
        for k in range(chunks)
    ]

    def spread(rows, row0, slots, slot0):
        at = lax.broadcasted_iota(jnp.int32, (rows, slots), 0) + row0
        frm = lax.broadcasted_iota(jnp.int32, (rows, slots), 1) + slot0
        same = at == CAP * (frm // PAD) + frm % PAD
        return (same & (frm % PAD < CAP)).astype(BF)

    arrived = [0]
    gate_copies = []

    def share_gates(k, pack, got):
        flat = jnp.dot(pack, got, preferred_element_type=F32).astype(BF)
        packed = jnp.zeros((PAD, 128), F32)
        e_at = lax.broadcasted_iota(jnp.int32, (128, 128), 0)
        l_at = lax.broadcasted_iota(jnp.int32, (128, 128), 1)
        for t in range(TILES[k]):
            move = ((e_at < experts) & (l_at == experts * t + e_at)).astype(BF)
            packed = packed + jnp.dot(
                flat[t * PAD : (t + 1) * PAD], move, preferred_element_type=F32
            )
        gp[k, 0] = packed.astype(BF)
        copies = []
        for dx, there in ((0, OWN), (1, LEFT), (3, RIGHT), (2, OPP)):
            for dc in (0, 1):
                if (dx, dc) == (0, 0):
                    continue
                n = len(copies)
                copy = remote(
                    gp.at[k, 0], gp.at[k, 4 * dc + there], gs_sem.at[k, n], gr_sem.at[k, n],
                    (me_n, dev_at(dx, dc)),
                )
                copy.start()
                copies.append(copy)
        gate_copies.append(copies)

    def deliver(k):
        lo, hi = bounds[k], bounds[k + 1]
        first, last = lo // CAP, min(N_OFF, (hi - 1) // CAP + 1)
        while arrived[0] < last - 1:
            arrived[0] += 1
            dispatch[arrived[0]].wait_recv()
        if k + 2 < len(WAVES):
            for r in range(WAVES[k + 1], WAVES[k + 2]):
                dispatch[r].start()
        pack = spread(hi - lo, lo, (last - first) * PAD, first * PAD)
        share_gates(k, pack, land[first:last, :, width:].reshape((last - first) * PAD, 128))

        def body(i, carry):
            cols = pl.ds(pl.multiple_of(i * step, step), step)
            got = land[first:last, :, cols].reshape((last - first) * PAD, step)
            xbuf[OWN, lo:hi, cols] = jnp.dot(pack, got, preferred_element_type=F32).astype(BF)
            return carry

        lax.fori_loop(0, width // step, body, 0, unroll=5)
        for j in (0, 1, 4):
            gather[k][j].start()

    def relay(k):
        gather[k][0].wait_recv()
        gather[k][2].start()
        gather[k][5].start()
        gather[k][1].wait_recv()
        gather[k][3].start()
        gather[k][6].start()

    def relay_opp(k):
        gather[k][2].wait_recv()
        gather[k][3].wait_recv()
        gather[k][7].start()

    def hidden(k):
        lo, hi = bounds[k], bounds[k + 1]
        m = 8 * (hi - lo)
        for j in (4, 5, 6, 7):
            gather[k][j].wait_recv()
        for copy in gate_copies[k]:
            copy.wait_recv()
        contract = (((1,), (1,)), ((), ()))
        columns = []
        for e in range(experts):
            pieces = []
            for s in range(8):
                for t in range(TILES[k]):
                    at = experts * t + e
                    pieces.append(gp[k, s, :, at : at + 1].astype(F32))
            columns.append(jnp.concatenate(pieces, axis=0))
        for e in range(experts):
            rows = xbuf[:, lo:hi, :].reshape(m, width)
            gate_val = lax.dot_general(rows, wg[e], contract, preferred_element_type=F32)
            up_val = lax.dot_general(rows, wu[e], contract, preferred_element_type=F32)
            act = gate_val / (1.0 + jnp.exp(-gate_val)) * up_val
            hid[e, 0:m, :] = (act * columns[e]).astype(BF)

    def reduce_copy(k, j, src, dst, cols, device, n=None):
        return remote(
            src.at[rows_of(k), cols], dst.at[rows_of(k), cols],
            rs_sem.at[k, j], rr_sem.at[k, j], (me_n, device),
        )

    reduce = [
        (
            remote(
                xbuf.at[4:8, rows_of(k), low], prbuf.at[:, rows_of(k), low],
                rs_sem.at[k, 0], rr_sem.at[k, 0], (me_n, to_core),
            ),
            remote(
                xbuf.at[4:8, rows_of(k), high], prbuf.at[:, rows_of(k), high],
                rs_sem.at[k, 1], rr_sem.at[k, 1], (me_n, to_core),
            ),
            reduce_copy(k, 2, xbuf.at[OPP, :, low], rabuf, low, to_right),
            reduce_copy(k, 3, xbuf.at[OPP, :, high], rbbuf, low, to_left),
            reduce_copy(k, 4, xbuf.at[RIGHT], flbuf, high, to_right),
            reduce_copy(k, 5, xbuf.at[LEFT], frbuf, low, to_left),
            reduce_copy(k, 6, xbuf.at[RIGHT], flbuf, low, to_right),
            reduce_copy(k, 7, xbuf.at[LEFT], frbuf, high, to_left),
        )
        for k in range(chunks)
    ]

    def project(k):
        lo, hi = bounds[k], bounds[k + 1]
        m = 8 * (hi - lo)
        for j in range(8):
            gather[k][j].wait_send()

        def body(i, carry):
            cols = pl.ds(pl.multiple_of(i * step, step), step)
            total = jnp.dot(hid[0, 0:m, :], wd[0, :, cols], preferred_element_type=F32)
            for e in range(1, experts):
                total += jnp.dot(hid[e, 0:m, :], wd[e, :, cols], preferred_element_type=F32)
            xbuf[:, lo:hi, cols] = total.astype(BF).reshape(8, hi - lo, step)
            return carry

        lax.fori_loop(0, half // step, body, 0)
        reduce[k][0].start()
        lax.fori_loop(half // step, width // step, body, 0)
        reduce[k][1].start()

    def add_up(k, place, start, others):
        lo, hi = bounds[k], bounds[k + 1]

        def body(i, carry):
            at = pl.multiple_of(i * step, step)
            cols = pl.ds(start + at, step)
            total = xbuf[place, lo:hi, cols].astype(F32)
            for other, shift in others:
                total += other[lo:hi, pl.ds(at + shift, step)].astype(F32)
            xbuf[place, lo:hi, cols] = total.astype(BF)
            return carry

        lax.fori_loop(0, half // step, body, 0)

    def pass_on(k):
        reduce[k][0].wait_recv()
        add_up(k, OPP, 0, ((prbuf.at[OPP], 0),))
        reduce[k][2].start()
        reduce[k][1].wait_recv()
        add_up(k, OPP, half, ((prbuf.at[OPP], half),))
        reduce[k][3].start()
        add_up(k, RIGHT, half, ((prbuf.at[RIGHT], half),))
        reduce[k][4].start()
        add_up(k, LEFT, 0, ((prbuf.at[LEFT], 0),))
        reduce[k][5].start()

    def pass_home(k):
        reduce[k][2].wait_recv()
        add_up(k, RIGHT, 0, ((prbuf.at[RIGHT], 0), (rabuf, 0)))
        reduce[k][6].start()
        reduce[k][3].wait_recv()
        add_up(k, LEFT, half, ((prbuf.at[LEFT], half), (rbbuf, 0)))
        reduce[k][7].start()

    returns = [None]
    returned = [0]

    def give_back(k):
        lo, hi = bounds[k], bounds[k + 1]
        for j in (4, 5, 6, 7):
            reduce[k][j].wait_recv()
        for start in (0, half):
            add_up(k, OWN, start, ((prbuf.at[OWN], start), (flbuf, start), (frbuf, start)))
        first, last = returned[0], hi // CAP
        returned[0] = last
        row0 = first * CAP // PAD * PAD
        unpack = (
            lax.broadcasted_iota(jnp.int32, ((last - first) * PAD, hi - row0), 1) + row0
        )
        frm = lax.broadcasted_iota(jnp.int32, ((last - first) * PAD, hi - row0), 0) + first * PAD
        unpack = ((unpack == CAP * (frm // PAD) + frm % PAD) & (frm % PAD < CAP)).astype(BF)
        own = 1 if first == 0 else 0

        def body(i, carry):
            cols = pl.ds(pl.multiple_of(i * step, step), step)
            back = jnp.dot(unpack, xbuf[OWN, row0:hi, cols], preferred_element_type=F32)
            back = back.astype(BF).reshape(last - first, PAD, step)
            if own:
                ret[0, :, cols] = back[0]
            send[first + own : last, :, cols] = back[own:]
            return carry

        lax.fori_loop(0, width // step, body, 0, unroll=5)
        for r in range(first + own, last):
            dz, dy = OFFS[r]
            copy = remote(
                send.at[r, :, all_cols], ret.at[r], bs_sem.at[r], br_sem.at[r],
                (node_at(-dz, -dy), me_d),
            )
            copy.start()
            returns.append(copy)

    deliver(0)
    relay(0)
    deliver(1)
    relay_opp(0)
    deliver(2)
    for load in loads:
        load.wait()
    hidden(0)
    relay(1)
    deliver(3)
    project(0)
    relay_opp(1)
    pass_on(0)
    relay(2)
    hidden(1)
    relay(3)
    relay_opp(2)
    project(1)
    pass_on(1)
    relay_opp(3)
    pass_home(0)
    hidden(2)
    project(2)
    pass_on(2)
    pass_home(1)
    hidden(3)
    project(3)
    for r in range(1, N_OFF):
        dispatch[r].wait_send()
    give_back(0)
    pass_home(2)
    pass_on(3)
    give_back(1)
    pass_home(3)
    give_back(2)
    give_back(3)

    for r in range(1, N_OFF):
        returns[r].wait_recv()
    outs = []
    parts = 2
    for p in range(parts):

        def combine(i, carry, p=p):
            cols = pl.ds(pl.multiple_of(p * (width // parts) + i * step, step), step)
            got = ret[:, :, cols].reshape(slots_all, step)
            total[:, cols] = jnp.dot(sel[...], got, preferred_element_type=F32).astype(BF)
            return carry

        lax.fori_loop(0, width // parts // step, combine, 0, unroll=5)
        cols = pl.ds(p * (width // parts), width // parts)
        copy = pltpu.make_async_copy(total.at[:, cols], out_ref.at[:, cols], o_sem.at[p])
        copy.start()
        outs.append(copy)

    for copies in gate_copies:
        for copy in copies:
            copy.wait_send()
    for k in range(chunks):
        for copy in reduce[k]:
            copy.wait_send()
    for r in range(1, N_OFF):
        returns[r].wait_send()
    for copy in outs:
        copy.wait()


def shards(tokens, node_ids, expert_pick, gate_share, gate_proj, up_proj, down_proj):
    toks, width = tokens.shape
    experts, units, _ = gate_proj.shape
    half = width // 2
    chunks = len(TILES)
    vmem = pl.BlockSpec(memory_space=pltpu.VMEM)
    hbm = pl.BlockSpec(memory_space=pl.ANY)
    dma = pltpu.SemaphoreType.DMA
    weights = pltpu.VMEM((experts, units, width), BF)
    return pl.pallas_call(
        kernel,
        out_shape=jax.ShapeDtypeStruct((toks, width), BF),
        in_specs=[vmem] * 4 + [hbm] * 3,
        out_specs=hbm,
        scratch_shapes=[
            weights,
            weights,
            weights,
            pltpu.VMEM((8, ROWS, width), BF),
            pltpu.VMEM((4, ROWS, width), BF),
            pltpu.VMEM((ROWS, half), BF),
            pltpu.VMEM((ROWS, half), BF),
            pltpu.VMEM((ROWS, width), BF),
            pltpu.VMEM((ROWS, width), BF),
            pltpu.VMEM((N_OFF, PAD, width + 128), BF),
            pltpu.VMEM((N_OFF, PAD, width + 128), BF),
            pltpu.VMEM((N_OFF, PAD, width), BF),
            pltpu.VMEM((experts, 8 * PAD * max(TILES), units), BF),
            pltpu.VMEM((chunks, 8, PAD, 128), BF),
            pltpu.VMEM((toks, N_OFF * PAD), BF),
            pltpu.VMEM((toks, width), BF),
            dma((2,)),
            dma((3,)),
            dma((N_OFF,)),
            dma((N_OFF,)),
            dma((chunks, 7)),
            dma((chunks, 7)),
            dma((chunks, 8)),
            dma((chunks, 8)),
            dma((chunks, 8)),
            dma((chunks, 8)),
            dma((N_OFF,)),
            dma((N_OFF,)),
        ],
        compiler_params=pltpu.CompilerParams(
            collective_id=0, has_side_effects=True, vmem_limit_bytes=67043328
        ),
    )(tokens, node_ids.T, expert_pick.T, gate_share.T, gate_proj, up_proj, down_proj)


def solution(mesh):
    return jax.shard_map(
        shards,
        mesh=mesh,
        in_specs=(
            P(("node", "dev"), None),
            P(("node", "dev"), None),
            P(("node", "dev"), None),
            P(("node", "dev"), None),
            P("node", "dev", None),
            P("node", "dev", None),
            P("node", "dev", None),
        ),
        out_specs=P(("node", "dev"), None),
        check_vma=False,
    )
```

```python
import functools

import jax
import jax.numpy as jnp
from jax import lax
from jax.experimental import pallas as pl
from jax.experimental.pallas import tpu as pltpu
from jax.sharding import PartitionSpec as P

MESH = pl.DeviceIdType.MESH
BF = jnp.bfloat16
F32 = jnp.float32

CAP = 13
PAD = 16
OFFS = (
    (0, 0), (0, 1), (1, 0), (3, 3),
    (2, 2), (1, 2), (2, 1), (3, 2),
    (0, 2), (2, 3), (2, 0), (3, 1), (1, 3),
    (1, 1), (3, 0), (0, 3),
)
N_OFF = len(OFFS)
WAVES = (1, 4, 9, N_OFF)
ROWS = N_OFF * CAP
TILES = (3, 4, 4, 2)
OWN, LEFT, RIGHT, OPP = 0, 1, 2, 3


def kernel(
    tok_ref, ids_ref, pick_ref, share_ref, wg_hbm, wu_hbm, wd_hbm, out_ref,
    wg, wu, wd, xbuf, prbuf, rabuf, rbbuf, flbuf, frbuf, send, land, ret, hid, gp, sel, total,
    o_sem, w_sem, ds_sem, dr_sem, gs_sem, gr_sem, as_sem, ar_sem, rs_sem, rr_sem, bs_sem, br_sem,
):
    toks, width = tok_ref.shape
    half = width // 2
    experts, units = wg.shape[0], wg.shape[1]
    chunks = len(TILES)
    bounds = [0]
    for t in TILES:
        bounds.append(bounds[-1] + t * PAD)
    step = min(512, half)
    slots_all = N_OFF * PAD

    me_n = lax.axis_index("node")
    me_d = lax.axis_index("dev")
    z, y = me_n // 4, me_n % 4
    x, c = me_d // 2, me_d % 2

    def node_at(dz, dy):
        return ((z + dz) % 4) * 4 + (y + dy) % 4

    def dev_at(dx, dc):
        return ((x + dx) % 4) * 2 + (c + dc) % 2

    to_right, to_left, to_core = dev_at(1, 0), dev_at(3, 0), dev_at(0, 1)

    loads = []
    for i, (src, dst) in enumerate(((wg_hbm, wg), (wu_hbm, wu), (wd_hbm, wd))):
        load = pltpu.make_async_copy(src, dst, w_sem.at[i])
        load.start()
        loads.append(load)

    barrier = pltpu.get_barrier_semaphore()
    peers = [(node_at(dz, dy), me_d) for dz, dy in OFFS[1:]]
    peers += [(me_n, dev_at(dx, dc)) for dx in range(4) for dc in range(2) if (dx, dc) != (0, 0)]
    for peer in peers:
        pl.semaphore_signal(barrier, inc=1, device_id=peer, device_id_type=MESH)

    def remote(src, dst, s_sem, r_sem, device):
        return pltpu.make_async_remote_copy(
            src_ref=src, dst_ref=dst, send_sem=s_sem, recv_sem=r_sem,
            device_id=device, device_id_type=MESH,
        )

    row = lax.broadcasted_iota(jnp.int32, (slots_all, toks), 0)
    block, slot = row // PAD, row % PAD
    dest = jnp.zeros((slots_all, toks), jnp.int32)
    for r, (dz, dy) in enumerate(OFFS):
        dest = jnp.where(block == r, node_at(dz, dy), dest)
    ids = ids_ref[...]
    choice = [(ids[k : k + 1, :] == dest).astype(F32) for k in range(ids.shape[0])]
    chosen = choice[0] + choice[1] + choice[2]
    earlier = (
        lax.broadcasted_iota(jnp.int32, (toks, toks), 0)
        < lax.broadcasted_iota(jnp.int32, (toks, toks), 1)
    ).astype(BF)
    rank = jnp.dot(chosen.astype(BF), earlier, preferred_element_type=F32)
    picked = jnp.where(rank == slot.astype(F32), chosen, 0.0)
    sel_t = picked.astype(BF)
    pick, share = pick_ref[...], share_ref[...].astype(F32)
    gates = jnp.zeros((slots_all, 128), F32)
    lane = lax.broadcasted_iota(jnp.int32, (toks, 128), 1)
    for e in range(experts):
        weight = jnp.zeros((slots_all, toks), F32)
        for k in range(len(choice)):
            part = jnp.sum(jnp.where(pick == k * experts + e, share, 0.0), axis=0, keepdims=True)
            weight = weight + choice[k] * part
        weight = (weight * picked).astype(BF)
        gates = gates + jnp.dot(weight, (lane == e).astype(BF), preferred_element_type=F32)
    send[:, :, width:] = gates.astype(BF).reshape(N_OFF, PAD, 128)

    def fill_send(i, carry):
        cols = pl.ds(pl.multiple_of(i * step, step), step)
        rows = jnp.dot(sel_t, tok_ref[:, cols], preferred_element_type=F32)
        send[:, :, cols] = rows.astype(BF).reshape(N_OFF, PAD, step)
        return carry

    lax.fori_loop(0, width // step, fill_send, 0)

    pl.semaphore_wait(barrier, len(peers))
    dispatch = [None]
    for r in range(1, N_OFF):
        copy = remote(
            send.at[r], land.at[r], ds_sem.at[r], dr_sem.at[r], (node_at(*OFFS[r]), me_d)
        )
        dispatch.append(copy)
    for r in range(WAVES[0], WAVES[1]):
        dispatch[r].start()
    land[0] = send[0]
    sel[...] = picked.T.astype(BF)

    def rows_of(k):
        return pl.ds(bounds[k], bounds[k + 1] - bounds[k])

    low, high = pl.ds(0, half), pl.ds(half, half)
    all_cols = pl.ds(0, width)

    def gather_copy(k, j, src, dst, cols, device):
        return remote(
            xbuf.at[src, rows_of(k), cols], xbuf.at[dst, rows_of(k), cols],
            as_sem.at[k, j], ar_sem.at[k, j], (me_n, device),
        )

    gather = [
        (
            gather_copy(k, 0, OWN, LEFT, all_cols, to_right),
            gather_copy(k, 1, OWN, RIGHT, all_cols, to_left),
            gather_copy(k, 2, LEFT, OPP, low, to_right),
            gather_copy(k, 3, RIGHT, OPP, high, to_left),
            gather_copy(k, 4, OWN, 4 + OWN, all_cols, to_core),
            gather_copy(k, 5, LEFT, 4 + LEFT, all_cols, to_core),
            gather_copy(k, 6, RIGHT, 4 + RIGHT, all_cols, to_core),
            gather_copy(k, 7, OPP, 4 + OPP, all_cols, to_core),
        )
        for k in range(chunks)
    ]

    def spread(rows, row0, slots, slot0):
        at = lax.broadcasted_iota(jnp.int32, (rows, slots), 0) + row0
        frm = lax.broadcasted_iota(jnp.int32, (rows, slots), 1) + slot0
        same = at == CAP * (frm // PAD) + frm % PAD
        return (same & (frm % PAD < CAP)).astype(BF)

    arrived = [0]
    gate_copies = []

    def share_gates(k, pack, got):
        flat = jnp.dot(pack, got, preferred_element_type=F32).astype(BF)
        packed = jnp.zeros((PAD, 128), F32)
        e_at = lax.broadcasted_iota(jnp.int32, (128, 128), 0)
        l_at = lax.broadcasted_iota(jnp.int32, (128, 128), 1)
        for t in range(TILES[k]):
            move = ((e_at < experts) & (l_at == experts * t + e_at)).astype(BF)
            packed = packed + jnp.dot(
                flat[t * PAD : (t + 1) * PAD], move, preferred_element_type=F32
            )
        gp[k, 0] = packed.astype(BF)
        copies = []
        for dx, there in ((0, OWN), (1, LEFT), (3, RIGHT), (2, OPP)):
            for dc in (0, 1):
                if (dx, dc) == (0, 0):
                    continue
                n = len(copies)
                copy = remote(
                    gp.at[k, 0], gp.at[k, 4 * dc + there], gs_sem.at[k, n], gr_sem.at[k, n],
                    (me_n, dev_at(dx, dc)),
                )
                copy.start()
                copies.append(copy)
        gate_copies.append(copies)

    def deliver(k):
        lo, hi = bounds[k], bounds[k + 1]
        first, last = lo // CAP, min(N_OFF, (hi - 1) // CAP + 1)
        while arrived[0] < last - 1:
            arrived[0] += 1
            dispatch[arrived[0]].wait_recv()
        if k + 2 < len(WAVES):
            for r in range(WAVES[k + 1], WAVES[k + 2]):
                dispatch[r].start()
        pack = spread(hi - lo, lo, (last - first) * PAD, first * PAD)
        share_gates(k, pack, land[first:last, :, width:].reshape((last - first) * PAD, 128))

        def body(i, carry):
            cols = pl.ds(pl.multiple_of(i * step, step), step)
            got = land[first:last, :, cols].reshape((last - first) * PAD, step)
            xbuf[OWN, lo:hi, cols] = jnp.dot(pack, got, preferred_element_type=F32).astype(BF)
            return carry

        lax.fori_loop(0, width // step, body, 0, unroll=5)
        for j in (0, 1, 4):
            gather[k][j].start()

    def relay(k):
        gather[k][0].wait_recv()
        gather[k][2].start()
        gather[k][5].start()
        gather[k][1].wait_recv()
        gather[k][3].start()
        gather[k][6].start()

    def relay_opp(k):
        gather[k][2].wait_recv()
        gather[k][3].wait_recv()
        gather[k][7].start()

    def hidden(k):
        lo, hi = bounds[k], bounds[k + 1]
        m = 8 * (hi - lo)
        for j in (4, 5, 6, 7):
            gather[k][j].wait_recv()
        for copy in gate_copies[k]:
            copy.wait_recv()
        contract = (((1,), (1,)), ((), ()))
        columns = []
        for e in range(experts):
            pieces = []
            for s in range(8):
                for t in range(TILES[k]):
                    at = experts * t + e
                    pieces.append(gp[k, s, :, at : at + 1].astype(F32))
            columns.append(jnp.concatenate(pieces, axis=0))
        for e in range(experts):
            rows = xbuf[:, lo:hi, :].reshape(m, width)
            gate_val = lax.dot_general(rows, wg[e], contract, preferred_element_type=F32)
            up_val = lax.dot_general(rows, wu[e], contract, preferred_element_type=F32)
            act = gate_val / (1.0 + jnp.exp(-gate_val)) * up_val
            hid[e, 0:m, :] = (act * columns[e]).astype(BF)

    def reduce_copy(k, j, src, dst, cols, device, n=None):
        return remote(
            src.at[rows_of(k), cols], dst.at[rows_of(k), cols],
            rs_sem.at[k, j], rr_sem.at[k, j], (me_n, device),
        )

    reduce = [
        (
            remote(
                xbuf.at[4:8, rows_of(k), low], prbuf.at[:, rows_of(k), low],
                rs_sem.at[k, 0], rr_sem.at[k, 0], (me_n, to_core),
            ),
            remote(
                xbuf.at[4:8, rows_of(k), high], prbuf.at[:, rows_of(k), high],
                rs_sem.at[k, 1], rr_sem.at[k, 1], (me_n, to_core),
            ),
            reduce_copy(k, 2, xbuf.at[OPP, :, low], rabuf, low, to_right),
            reduce_copy(k, 3, xbuf.at[OPP, :, high], rbbuf, low, to_left),
            reduce_copy(k, 4, xbuf.at[RIGHT], flbuf, high, to_right),
            reduce_copy(k, 5, xbuf.at[LEFT], frbuf, low, to_left),
            reduce_copy(k, 6, xbuf.at[RIGHT], flbuf, low, to_right),
            reduce_copy(k, 7, xbuf.at[LEFT], frbuf, high, to_left),
        )
        for k in range(chunks)
    ]

    def project(k):
        lo, hi = bounds[k], bounds[k + 1]
        m = 8 * (hi - lo)
        for j in range(8):
            gather[k][j].wait_send()

        def body(i, carry):
            cols = pl.ds(pl.multiple_of(i * step, step), step)
            total = jnp.dot(hid[0, 0:m, :], wd[0, :, cols], preferred_element_type=F32)
            for e in range(1, experts):
                total += jnp.dot(hid[e, 0:m, :], wd[e, :, cols], preferred_element_type=F32)
            xbuf[:, lo:hi, cols] = total.astype(BF).reshape(8, hi - lo, step)
            return carry

        lax.fori_loop(0, half // step, body, 0)
        reduce[k][0].start()
        lax.fori_loop(half // step, width // step, body, 0)
        reduce[k][1].start()

    def add_up(k, place, start, others):
        lo, hi = bounds[k], bounds[k + 1]

        def body(i, carry):
            at = pl.multiple_of(i * step, step)
            cols = pl.ds(start + at, step)
            total = xbuf[place, lo:hi, cols].astype(F32)
            for other, shift in others:
                total += other[lo:hi, pl.ds(at + shift, step)].astype(F32)
            xbuf[place, lo:hi, cols] = total.astype(BF)
            return carry

        lax.fori_loop(0, half // step, body, 0)

    def pass_on(k):
        reduce[k][0].wait_recv()
        add_up(k, OPP, 0, ((prbuf.at[OPP], 0),))
        reduce[k][2].start()
        reduce[k][1].wait_recv()
        add_up(k, OPP, half, ((prbuf.at[OPP], half),))
        reduce[k][3].start()
        add_up(k, RIGHT, half, ((prbuf.at[RIGHT], half),))
        reduce[k][4].start()
        add_up(k, LEFT, 0, ((prbuf.at[LEFT], 0),))
        reduce[k][5].start()

    def pass_home(k):
        reduce[k][2].wait_recv()
        add_up(k, RIGHT, 0, ((prbuf.at[RIGHT], 0), (rabuf, 0)))
        reduce[k][6].start()
        reduce[k][3].wait_recv()
        add_up(k, LEFT, half, ((prbuf.at[LEFT], half), (rbbuf, 0)))
        reduce[k][7].start()

    returns = [None]
    returned = [0]

    def give_back(k):
        lo, hi = bounds[k], bounds[k + 1]
        for j in (4, 5, 6, 7):
            reduce[k][j].wait_recv()
        for start in (0, half):
            add_up(k, OWN, start, ((prbuf.at[OWN], start), (flbuf, start), (frbuf, start)))
        first, last = returned[0], hi // CAP
        returned[0] = last
        row0 = first * CAP // PAD * PAD
        unpack = (
            lax.broadcasted_iota(jnp.int32, ((last - first) * PAD, hi - row0), 1) + row0
        )
        frm = lax.broadcasted_iota(jnp.int32, ((last - first) * PAD, hi - row0), 0) + first * PAD
        unpack = ((unpack == CAP * (frm // PAD) + frm % PAD) & (frm % PAD < CAP)).astype(BF)
        own = 1 if first == 0 else 0

        def body(i, carry):
            cols = pl.ds(pl.multiple_of(i * step, step), step)
            back = jnp.dot(unpack, xbuf[OWN, row0:hi, cols], preferred_element_type=F32)
            back = back.astype(BF).reshape(last - first, PAD, step)
            if own:
                ret[0, :, cols] = back[0]
            send[first + own : last, :, cols] = back[own:]
            return carry

        lax.fori_loop(0, width // step, body, 0, unroll=5)
        for r in range(first + own, last):
            dz, dy = OFFS[r]
            copy = remote(
                send.at[r, :, all_cols], ret.at[r], bs_sem.at[r], br_sem.at[r],
                (node_at(-dz, -dy), me_d),
            )
            copy.start()
            returns.append(copy)

    deliver(0)
    relay(0)
    deliver(1)
    relay_opp(0)
    for load in loads:
        load.wait()
    hidden(0)
    project(0)
    pass_on(0)
    relay(1)
    pass_home(0)
    deliver(2)
    relay_opp(1)
    hidden(1)
    project(1)
    pass_on(1)
    relay(2)
    for r in range(1, N_OFF):
        dispatch[r].wait_send()
    give_back(0)
    pass_home(1)
    deliver(3)
    relay_opp(2)
    hidden(2)
    project(2)
    relay(3)
    pass_on(2)
    give_back(1)
    relay_opp(3)
    hidden(3)
    project(3)
    pass_home(2)
    pass_on(3)
    pass_home(3)
    give_back(2)
    give_back(3)

    for r in range(1, N_OFF):
        returns[r].wait_recv()
    outs = []
    parts = 2
    for p in range(parts):

        def combine(i, carry, p=p):
            cols = pl.ds(pl.multiple_of(p * (width // parts) + i * step, step), step)
            got = ret[:, :, cols].reshape(slots_all, step)
            total[:, cols] = jnp.dot(sel[...], got, preferred_element_type=F32).astype(BF)
            return carry

        lax.fori_loop(0, width // parts // step, combine, 0, unroll=5)
        cols = pl.ds(p * (width // parts), width // parts)
        copy = pltpu.make_async_copy(total.at[:, cols], out_ref.at[:, cols], o_sem.at[p])
        copy.start()
        outs.append(copy)

    for copies in gate_copies:
        for copy in copies:
            copy.wait_send()
    for k in range(chunks):
        for copy in reduce[k]:
            copy.wait_send()
    for r in range(1, N_OFF):
        returns[r].wait_send()
    for copy in outs:
        copy.wait()


def shards(tokens, node_ids, expert_pick, gate_share, gate_proj, up_proj, down_proj):
    toks, width = tokens.shape
    experts, units, _ = gate_proj.shape
    half = width // 2
    chunks = len(TILES)
    vmem = pl.BlockSpec(memory_space=pltpu.VMEM)
    hbm = pl.BlockSpec(memory_space=pl.ANY)
    dma = pltpu.SemaphoreType.DMA
    weights = pltpu.VMEM((experts, units, width), BF)
    return pl.pallas_call(
        kernel,
        out_shape=jax.ShapeDtypeStruct((toks, width), BF),
        in_specs=[vmem] * 4 + [hbm] * 3,
        out_specs=hbm,
        scratch_shapes=[
            weights,
            weights,
            weights,
            pltpu.VMEM((8, ROWS, width), BF),
            pltpu.VMEM((4, ROWS, width), BF),
            pltpu.VMEM((ROWS, half), BF),
            pltpu.VMEM((ROWS, half), BF),
            pltpu.VMEM((ROWS, width), BF),
            pltpu.VMEM((ROWS, width), BF),
            pltpu.VMEM((N_OFF, PAD, width + 128), BF),
            pltpu.VMEM((N_OFF, PAD, width + 128), BF),
            pltpu.VMEM((N_OFF, PAD, width), BF),
            pltpu.VMEM((experts, 8 * PAD * max(TILES), units), BF),
            pltpu.VMEM((chunks, 8, PAD, 128), BF),
            pltpu.VMEM((toks, N_OFF * PAD), BF),
            pltpu.VMEM((toks, width), BF),
            dma((2,)),
            dma((3,)),
            dma((N_OFF,)),
            dma((N_OFF,)),
            dma((chunks, 7)),
            dma((chunks, 7)),
            dma((chunks, 8)),
            dma((chunks, 8)),
            dma((chunks, 8)),
            dma((chunks, 8)),
            dma((N_OFF,)),
            dma((N_OFF,)),
        ],
        compiler_params=pltpu.CompilerParams(
            collective_id=0, has_side_effects=True, vmem_limit_bytes=67043328
        ),
    )(tokens, node_ids.T, expert_pick.T, gate_share.T, gate_proj, up_proj, down_proj)


def solution(mesh):
    return jax.shard_map(
        shards,
        mesh=mesh,
        in_specs=(
            P(("node", "dev"), None),
            P(("node", "dev"), None),
            P(("node", "dev"), None),
            P(("node", "dev"), None),
            P("node", "dev", None),
            P("node", "dev", None),
            P("node", "dev", None),
        ),
        out_specs=P(("node", "dev"), None),
        check_vma=False,
    )
```

```python
import functools

import jax
import jax.numpy as jnp
from jax import lax
from jax.experimental import pallas as pl
from jax.experimental.pallas import tpu as pltpu
from jax.sharding import PartitionSpec as P

MESH = pl.DeviceIdType.MESH
BF = jnp.bfloat16
F32 = jnp.float32

CAP = 13
PAD = 16
OFFS = (
    (0, 0), (0, 1), (1, 0), (3, 3),
    (2, 2), (1, 2), (2, 1), (3, 2),
    (0, 2), (2, 3), (2, 0), (3, 1), (1, 3),
    (1, 1), (3, 0), (0, 3),
)
N_OFF = len(OFFS)
WAVES = (1, 9, 9, N_OFF)
ROWS = N_OFF * CAP
TILES = (3, 4, 4, 2)
OWN, LEFT, RIGHT, OPP = 0, 1, 2, 3


def kernel(
    tok_ref, ids_ref, pick_ref, share_ref, wg_hbm, wu_hbm, wd_hbm, out_ref,
    wg, wu, wd, xbuf, prbuf, rabuf, rbbuf, flbuf, frbuf, send, land, ret, hid, gp, sel, total,
    o_sem, w_sem, ds_sem, dr_sem, gs_sem, gr_sem, as_sem, ar_sem, rs_sem, rr_sem, bs_sem, br_sem,
):
    toks, width = tok_ref.shape
    half = width // 2
    experts, units = wg.shape[0], wg.shape[1]
    chunks = len(TILES)
    bounds = [0]
    for t in TILES:
        bounds.append(bounds[-1] + t * PAD)
    step = min(512, half)
    slots_all = N_OFF * PAD

    me_n = lax.axis_index("node")
    me_d = lax.axis_index("dev")
    z, y = me_n // 4, me_n % 4
    x, c = me_d // 2, me_d % 2

    def node_at(dz, dy):
        return ((z + dz) % 4) * 4 + (y + dy) % 4

    def dev_at(dx, dc):
        return ((x + dx) % 4) * 2 + (c + dc) % 2

    to_right, to_left, to_core = dev_at(1, 0), dev_at(3, 0), dev_at(0, 1)

    loads = []
    for i, (src, dst) in enumerate(((wg_hbm, wg), (wu_hbm, wu), (wd_hbm, wd))):
        load = pltpu.make_async_copy(src, dst, w_sem.at[i])
        load.start()
        loads.append(load)

    barrier = pltpu.get_barrier_semaphore()
    peers = [(node_at(dz, dy), me_d) for dz, dy in OFFS[1:]]
    peers += [(me_n, dev_at(dx, dc)) for dx in range(4) for dc in range(2) if (dx, dc) != (0, 0)]
    for peer in peers:
        pl.semaphore_signal(barrier, inc=1, device_id=peer, device_id_type=MESH)

    def remote(src, dst, s_sem, r_sem, device):
        return pltpu.make_async_remote_copy(
            src_ref=src, dst_ref=dst, send_sem=s_sem, recv_sem=r_sem,
            device_id=device, device_id_type=MESH,
        )

    row = lax.broadcasted_iota(jnp.int32, (slots_all, toks), 0)
    block, slot = row // PAD, row % PAD
    dest = jnp.zeros((slots_all, toks), jnp.int32)
    for r, (dz, dy) in enumerate(OFFS):
        dest = jnp.where(block == r, node_at(dz, dy), dest)
    ids = ids_ref[...]
    choice = [(ids[k : k + 1, :] == dest).astype(F32) for k in range(ids.shape[0])]
    chosen = choice[0] + choice[1] + choice[2]
    earlier = (
        lax.broadcasted_iota(jnp.int32, (toks, toks), 0)
        < lax.broadcasted_iota(jnp.int32, (toks, toks), 1)
    ).astype(BF)
    rank = jnp.dot(chosen.astype(BF), earlier, preferred_element_type=F32)
    picked = jnp.where(rank == slot.astype(F32), chosen, 0.0)
    sel_t = picked.astype(BF)
    pick, share = pick_ref[...], share_ref[...].astype(F32)
    gates = jnp.zeros((slots_all, 128), F32)
    lane = lax.broadcasted_iota(jnp.int32, (toks, 128), 1)
    for e in range(experts):
        weight = jnp.zeros((slots_all, toks), F32)
        for k in range(len(choice)):
            part = jnp.sum(jnp.where(pick == k * experts + e, share, 0.0), axis=0, keepdims=True)
            weight = weight + choice[k] * part
        weight = (weight * picked).astype(BF)
        gates = gates + jnp.dot(weight, (lane == e).astype(BF), preferred_element_type=F32)
    send[:, :, width:] = gates.astype(BF).reshape(N_OFF, PAD, 128)

    def fill_send(i, carry):
        cols = pl.ds(pl.multiple_of(i * step, step), step)
        rows = jnp.dot(sel_t, tok_ref[:, cols], preferred_element_type=F32)
        send[:, :, cols] = rows.astype(BF).reshape(N_OFF, PAD, step)
        return carry

    lax.fori_loop(0, width // step, fill_send, 0)

    pl.semaphore_wait(barrier, len(peers))
    dispatch = [None]
    for r in range(1, N_OFF):
        copy = remote(
            send.at[r], land.at[r], ds_sem.at[r], dr_sem.at[r], (node_at(*OFFS[r]), me_d)
        )
        dispatch.append(copy)
    for r in range(WAVES[0], WAVES[1]):
        dispatch[r].start()
    land[0] = send[0]
    sel[...] = picked.T.astype(BF)

    def rows_of(k):
        return pl.ds(bounds[k], bounds[k + 1] - bounds[k])

    low, high = pl.ds(0, half), pl.ds(half, half)
    all_cols = pl.ds(0, width)

    def gather_copy(k, j, src, dst, cols, device):
        return remote(
            xbuf.at[src, rows_of(k), cols], xbuf.at[dst, rows_of(k), cols],
            as_sem.at[k, j], ar_sem.at[k, j], (me_n, device),
        )

    gather = [
        (
            gather_copy(k, 0, OWN, LEFT, all_cols, to_right),
            gather_copy(k, 1, OWN, RIGHT, all_cols, to_left),
            gather_copy(k, 2, LEFT, OPP, low, to_right),
            gather_copy(k, 3, RIGHT, OPP, high, to_left),
            gather_copy(k, 4, OWN, 4 + OWN, all_cols, to_core),
            gather_copy(k, 5, LEFT, 4 + LEFT, all_cols, to_core),
            gather_copy(k, 6, RIGHT, 4 + RIGHT, all_cols, to_core),
            gather_copy(k, 7, OPP, 4 + OPP, all_cols, to_core),
        )
        for k in range(chunks)
    ]

    def spread(rows, row0, slots, slot0):
        at = lax.broadcasted_iota(jnp.int32, (rows, slots), 0) + row0
        frm = lax.broadcasted_iota(jnp.int32, (rows, slots), 1) + slot0
        same = at == CAP * (frm // PAD) + frm % PAD
        return (same & (frm % PAD < CAP)).astype(BF)

    arrived = [0]
    gate_copies = []

    def share_gates(k, pack, got):
        flat = jnp.dot(pack, got, preferred_element_type=F32).astype(BF)
        packed = jnp.zeros((PAD, 128), F32)
        e_at = lax.broadcasted_iota(jnp.int32, (128, 128), 0)
        l_at = lax.broadcasted_iota(jnp.int32, (128, 128), 1)
        for t in range(TILES[k]):
            move = ((e_at < experts) & (l_at == experts * t + e_at)).astype(BF)
            packed = packed + jnp.dot(
                flat[t * PAD : (t + 1) * PAD], move, preferred_element_type=F32
            )
        gp[k, 0] = packed.astype(BF)
        copies = []
        for dx, there in ((0, OWN), (1, LEFT), (3, RIGHT), (2, OPP)):
            for dc in (0, 1):
                if (dx, dc) == (0, 0):
                    continue
                n = len(copies)
                copy = remote(
                    gp.at[k, 0], gp.at[k, 4 * dc + there], gs_sem.at[k, n], gr_sem.at[k, n],
                    (me_n, dev_at(dx, dc)),
                )
                copy.start()
                copies.append(copy)
        gate_copies.append(copies)

    def deliver(k):
        lo, hi = bounds[k], bounds[k + 1]
        first, last = lo // CAP, min(N_OFF, (hi - 1) // CAP + 1)
        while arrived[0] < last - 1:
            arrived[0] += 1
            dispatch[arrived[0]].wait_recv()
        if k + 2 < len(WAVES):
            for r in range(WAVES[k + 1], WAVES[k + 2]):
                dispatch[r].start()
        pack = spread(hi - lo, lo, (last - first) * PAD, first * PAD)
        share_gates(k, pack, land[first:last, :, width:].reshape((last - first) * PAD, 128))

        def body(i, carry):
            cols = pl.ds(pl.multiple_of(i * step, step), step)
            got = land[first:last, :, cols].reshape((last - first) * PAD, step)
            xbuf[OWN, lo:hi, cols] = jnp.dot(pack, got, preferred_element_type=F32).astype(BF)
            return carry

        lax.fori_loop(0, width // step, body, 0, unroll=5)
        for j in (0, 1, 4):
            gather[k][j].start()

    def relay(k):
        gather[k][0].wait_recv()
        gather[k][2].start()
        gather[k][5].start()
        gather[k][1].wait_recv()
        gather[k][3].start()
        gather[k][6].start()

    def relay_opp(k):
        gather[k][2].wait_recv()
        gather[k][3].wait_recv()
        gather[k][7].start()

    def hidden(k):
        lo, hi = bounds[k], bounds[k + 1]
        m = 8 * (hi - lo)
        for j in (4, 5, 6, 7):
            gather[k][j].wait_recv()
        for copy in gate_copies[k]:
            copy.wait_recv()
        contract = (((1,), (1,)), ((), ()))
        columns = []
        for e in range(experts):
            pieces = []
            for s in range(8):
                for t in range(TILES[k]):
                    at = experts * t + e
                    pieces.append(gp[k, s, :, at : at + 1].astype(F32))
            columns.append(jnp.concatenate(pieces, axis=0))
        for e in range(experts):
            rows = xbuf[:, lo:hi, :].reshape(m, width)
            gate_val = lax.dot_general(rows, wg[e], contract, preferred_element_type=F32)
            up_val = lax.dot_general(rows, wu[e], contract, preferred_element_type=F32)
            act = gate_val / (1.0 + jnp.exp(-gate_val)) * up_val
            hid[e, 0:m, :] = (act * columns[e]).astype(BF)

    def reduce_copy(k, j, src, dst, cols, device, n=None):
        return remote(
            src.at[rows_of(k), cols], dst.at[rows_of(k), cols],
            rs_sem.at[k, j], rr_sem.at[k, j], (me_n, device),
        )

    reduce = [
        (
            remote(
                xbuf.at[4:8, rows_of(k), low], prbuf.at[:, rows_of(k), low],
                rs_sem.at[k, 0], rr_sem.at[k, 0], (me_n, to_core),
            ),
            remote(
                xbuf.at[4:8, rows_of(k), high], prbuf.at[:, rows_of(k), high],
                rs_sem.at[k, 1], rr_sem.at[k, 1], (me_n, to_core),
            ),
            reduce_copy(k, 2, xbuf.at[OPP, :, low], rabuf, low, to_right),
            reduce_copy(k, 3, xbuf.at[OPP, :, high], rbbuf, low, to_left),
            reduce_copy(k, 4, xbuf.at[RIGHT], flbuf, high, to_right),
            reduce_copy(k, 5, xbuf.at[LEFT], frbuf, low, to_left),
            reduce_copy(k, 6, xbuf.at[RIGHT], flbuf, low, to_right),
            reduce_copy(k, 7, xbuf.at[LEFT], frbuf, high, to_left),
        )
        for k in range(chunks)
    ]

    def project(k):
        lo, hi = bounds[k], bounds[k + 1]
        m = 8 * (hi - lo)
        for j in range(8):
            gather[k][j].wait_send()

        def body(i, carry):
            cols = pl.ds(pl.multiple_of(i * step, step), step)
            total = jnp.dot(hid[0, 0:m, :], wd[0, :, cols], preferred_element_type=F32)
            for e in range(1, experts):
                total += jnp.dot(hid[e, 0:m, :], wd[e, :, cols], preferred_element_type=F32)
            xbuf[:, lo:hi, cols] = total.astype(BF).reshape(8, hi - lo, step)
            return carry

        lax.fori_loop(0, half // step, body, 0)
        reduce[k][0].start()
        lax.fori_loop(half // step, width // step, body, 0)
        reduce[k][1].start()

    def add_up(k, place, start, others):
        lo, hi = bounds[k], bounds[k + 1]

        def body(i, carry):
            at = pl.multiple_of(i * step, step)
            cols = pl.ds(start + at, step)
            total = xbuf[place, lo:hi, cols].astype(F32)
            for other, shift in others:
                total += other[lo:hi, pl.ds(at + shift, step)].astype(F32)
            xbuf[place, lo:hi, cols] = total.astype(BF)
            return carry

        lax.fori_loop(0, half // step, body, 0)

    def pass_on(k):
        reduce[k][0].wait_recv()
        add_up(k, OPP, 0, ((prbuf.at[OPP], 0),))
        reduce[k][2].start()
        reduce[k][1].wait_recv()
        add_up(k, OPP, half, ((prbuf.at[OPP], half),))
        reduce[k][3].start()
        add_up(k, RIGHT, half, ((prbuf.at[RIGHT], half),))
        reduce[k][4].start()
        add_up(k, LEFT, 0, ((prbuf.at[LEFT], 0),))
        reduce[k][5].start()

    def pass_home(k):
        reduce[k][2].wait_recv()
        add_up(k, RIGHT, 0, ((prbuf.at[RIGHT], 0), (rabuf, 0)))
        reduce[k][6].start()
        reduce[k][3].wait_recv()
        add_up(k, LEFT, half, ((prbuf.at[LEFT], half), (rbbuf, 0)))
        reduce[k][7].start()

    returns = [None]
    returned = [0]

    def give_back(k):
        lo, hi = bounds[k], bounds[k + 1]
        for j in (4, 5, 6, 7):
            reduce[k][j].wait_recv()
        for start in (0, half):
            add_up(k, OWN, start, ((prbuf.at[OWN], start), (flbuf, start), (frbuf, start)))
        first, last = returned[0], hi // CAP
        returned[0] = last
        row0 = first * CAP // PAD * PAD
        unpack = (
            lax.broadcasted_iota(jnp.int32, ((last - first) * PAD, hi - row0), 1) + row0
        )
        frm = lax.broadcasted_iota(jnp.int32, ((last - first) * PAD, hi - row0), 0) + first * PAD
        unpack = ((unpack == CAP * (frm // PAD) + frm % PAD) & (frm % PAD < CAP)).astype(BF)
        own = 1 if first == 0 else 0

        def body(i, carry):
            cols = pl.ds(pl.multiple_of(i * step, step), step)
            back = jnp.dot(unpack, xbuf[OWN, row0:hi, cols], preferred_element_type=F32)
            back = back.astype(BF).reshape(last - first, PAD, step)
            if own:
                ret[0, :, cols] = back[0]
            send[first + own : last, :, cols] = back[own:]
            return carry

        lax.fori_loop(0, width // step, body, 0, unroll=5)
        for r in range(first + own, last):
            dz, dy = OFFS[r]
            copy = remote(
                send.at[r, :, all_cols], ret.at[r], bs_sem.at[r], br_sem.at[r],
                (node_at(-dz, -dy), me_d),
            )
            copy.start()
            returns.append(copy)

    deliver(0)
    relay(0)
    deliver(1)
    relay_opp(0)
    for load in loads:
        load.wait()
    hidden(0)
    project(0)
    pass_on(0)
    relay(1)
    deliver(2)
    pass_home(0)
    deliver(3)
    relay_opp(1)
    hidden(1)
    project(1)
    relay(2)
    pass_on(1)
    for r in range(1, N_OFF):
        dispatch[r].wait_send()
    give_back(0)
    relay(3)
    relay_opp(2)
    hidden(2)
    pass_home(1)
    project(2)
    pass_on(2)
    relay_opp(3)
    hidden(3)
    project(3)
    give_back(1)
    pass_home(2)
    pass_on(3)
    give_back(2)
    pass_home(3)
    give_back(3)

    for r in range(1, N_OFF):
        returns[r].wait_recv()
    outs = []
    parts = 2
    for p in range(parts):

        def combine(i, carry, p=p):
            cols = pl.ds(pl.multiple_of(p * (width // parts) + i * step, step), step)
            got = ret[:, :, cols].reshape(slots_all, step)
            total[:, cols] = jnp.dot(sel[...], got, preferred_element_type=F32).astype(BF)
            return carry

        lax.fori_loop(0, width // parts // step, combine, 0, unroll=5)
        cols = pl.ds(p * (width // parts), width // parts)
        copy = pltpu.make_async_copy(total.at[:, cols], out_ref.at[:, cols], o_sem.at[p])
        copy.start()
        outs.append(copy)

    for copies in gate_copies:
        for copy in copies:
            copy.wait_send()
    for k in range(chunks):
        for copy in reduce[k]:
            copy.wait_send()
    for r in range(1, N_OFF):
        returns[r].wait_send()
    for copy in outs:
        copy.wait()


def shards(tokens, node_ids, expert_pick, gate_share, gate_proj, up_proj, down_proj):
    toks, width = tokens.shape
    experts, units, _ = gate_proj.shape
    half = width // 2
    chunks = len(TILES)
    vmem = pl.BlockSpec(memory_space=pltpu.VMEM)
    hbm = pl.BlockSpec(memory_space=pl.ANY)
    dma = pltpu.SemaphoreType.DMA
    weights = pltpu.VMEM((experts, units, width), BF)
    return pl.pallas_call(
        kernel,
        out_shape=jax.ShapeDtypeStruct((toks, width), BF),
        in_specs=[vmem] * 4 + [hbm] * 3,
        out_specs=hbm,
        scratch_shapes=[
            weights,
            weights,
            weights,
            pltpu.VMEM((8, ROWS, width), BF),
            pltpu.VMEM((4, ROWS, width), BF),
            pltpu.VMEM((ROWS, half), BF),
            pltpu.VMEM((ROWS, half), BF),
            pltpu.VMEM((ROWS, width), BF),
            pltpu.VMEM((ROWS, width), BF),
            pltpu.VMEM((N_OFF, PAD, width + 128), BF),
            pltpu.VMEM((N_OFF, PAD, width + 128), BF),
            pltpu.VMEM((N_OFF, PAD, width), BF),
            pltpu.VMEM((experts, 8 * PAD * max(TILES), units), BF),
            pltpu.VMEM((chunks, 8, PAD, 128), BF),
            pltpu.VMEM((toks, N_OFF * PAD), BF),
            pltpu.VMEM((toks, width), BF),
            dma((2,)),
            dma((3,)),
            dma((N_OFF,)),
            dma((N_OFF,)),
            dma((chunks, 7)),
            dma((chunks, 7)),
            dma((chunks, 8)),
            dma((chunks, 8)),
            dma((chunks, 8)),
            dma((chunks, 8)),
            dma((N_OFF,)),
            dma((N_OFF,)),
        ],
        compiler_params=pltpu.CompilerParams(
            collective_id=0, has_side_effects=True, vmem_limit_bytes=67043328
        ),
    )(tokens, node_ids.T, expert_pick.T, gate_share.T, gate_proj, up_proj, down_proj)


def solution(mesh):
    return jax.shard_map(
        shards,
        mesh=mesh,
        in_specs=(
            P(("node", "dev"), None),
            P(("node", "dev"), None),
            P(("node", "dev"), None),
            P(("node", "dev"), None),
            P("node", "dev", None),
            P("node", "dev", None),
            P("node", "dev", None),
        ),
        out_specs=P(("node", "dev"), None),
        check_vma=False,
    )
```

```python
import functools

import jax
import jax.numpy as jnp
from jax import lax
from jax.experimental import pallas as pl
from jax.experimental.pallas import tpu as pltpu
from jax.sharding import PartitionSpec as P

MESH = pl.DeviceIdType.MESH
BF = jnp.bfloat16
F32 = jnp.float32

CAP = 13
PAD = 16
OFFS = (
    (0, 0), (0, 1), (1, 0), (3, 3),
    (2, 2), (1, 2), (2, 1), (3, 2),
    (0, 2), (2, 3), (2, 0), (3, 1), (1, 3),
    (1, 1), (3, 0), (0, 3),
)
N_OFF = len(OFFS)
WAVES = (1, 4, 9, N_OFF)
ROWS = N_OFF * CAP
TILES = (3, 4, 4, 2)
OWN, LEFT, RIGHT, OPP = 0, 1, 2, 3


def kernel(
    tok_ref, ids_ref, pick_ref, share_ref, wg_hbm, wu_hbm, wd_hbm, out_ref,
    wg, wu, wd, xbuf, prbuf, rabuf, rbbuf, flbuf, frbuf, send, land, ret, hid, gp, sel, total,
    o_sem, w_sem, ds_sem, dr_sem, gs_sem, gr_sem, as_sem, ar_sem, rs_sem, rr_sem, bs_sem, br_sem,
):
    toks, width = tok_ref.shape
    half = width // 2
    experts, units = wg.shape[0], wg.shape[1]
    chunks = len(TILES)
    bounds = [0]
    for t in TILES:
        bounds.append(bounds[-1] + t * PAD)
    step = min(512, half)
    slots_all = N_OFF * PAD

    me_n = lax.axis_index("node")
    me_d = lax.axis_index("dev")
    z, y = me_n // 4, me_n % 4
    x, c = me_d // 2, me_d % 2

    def node_at(dz, dy):
        return ((z + dz) % 4) * 4 + (y + dy) % 4

    def dev_at(dx, dc):
        return ((x + dx) % 4) * 2 + (c + dc) % 2

    to_right, to_left, to_core = dev_at(1, 0), dev_at(3, 0), dev_at(0, 1)

    loads = []
    for i, (src, dst) in enumerate(((wg_hbm, wg), (wu_hbm, wu), (wd_hbm, wd))):
        load = pltpu.make_async_copy(src, dst, w_sem.at[i])
        load.start()
        loads.append(load)

    barrier = pltpu.get_barrier_semaphore()
    peers = [(node_at(dz, dy), me_d) for dz, dy in OFFS[1:]]
    peers += [(me_n, dev_at(dx, dc)) for dx in range(4) for dc in range(2) if (dx, dc) != (0, 0)]
    for peer in peers:
        pl.semaphore_signal(barrier, inc=1, device_id=peer, device_id_type=MESH)

    def remote(src, dst, s_sem, r_sem, device):
        return pltpu.make_async_remote_copy(
            src_ref=src, dst_ref=dst, send_sem=s_sem, recv_sem=r_sem,
            device_id=device, device_id_type=MESH,
        )

    row = lax.broadcasted_iota(jnp.int32, (slots_all, toks), 0)
    block, slot = row // PAD, row % PAD
    dest = jnp.zeros((slots_all, toks), jnp.int32)
    for r, (dz, dy) in enumerate(OFFS):
        dest = jnp.where(block == r, node_at(dz, dy), dest)
    ids = ids_ref[...]
    choice = [(ids[k : k + 1, :] == dest).astype(F32) for k in range(ids.shape[0])]
    chosen = choice[0] + choice[1] + choice[2]
    earlier = (
        lax.broadcasted_iota(jnp.int32, (toks, toks), 0)
        < lax.broadcasted_iota(jnp.int32, (toks, toks), 1)
    ).astype(BF)
    rank = jnp.dot(chosen.astype(BF), earlier, preferred_element_type=F32)
    picked = jnp.where(rank == slot.astype(F32), chosen, 0.0)
    sel_t = picked.astype(BF)
    pick, share = pick_ref[...], share_ref[...].astype(F32)
    gates = jnp.zeros((slots_all, 128), F32)
    lane = lax.broadcasted_iota(jnp.int32, (toks, 128), 1)
    for e in range(experts):
        weight = jnp.zeros((slots_all, toks), F32)
        for k in range(len(choice)):
            part = jnp.sum(jnp.where(pick == k * experts + e, share, 0.0), axis=0, keepdims=True)
            weight = weight + choice[k] * part
        weight = (weight * picked).astype(BF)
        gates = gates + jnp.dot(weight, (lane == e).astype(BF), preferred_element_type=F32)
    send[:, :, width:] = gates.astype(BF).reshape(N_OFF, PAD, 128)

    def fill_send(i, carry):
        cols = pl.ds(pl.multiple_of(i * step, step), step)
        rows = jnp.dot(sel_t, tok_ref[:, cols], preferred_element_type=F32)
        send[:, :, cols] = rows.astype(BF).reshape(N_OFF, PAD, step)
        return carry

    lax.fori_loop(0, width // step, fill_send, 0)

    pl.semaphore_wait(barrier, len(peers))
    dispatch = [None]
    for r in range(1, N_OFF):
        copy = remote(
            send.at[r], land.at[r], ds_sem.at[r], dr_sem.at[r], (node_at(*OFFS[r]), me_d)
        )
        dispatch.append(copy)
    for r in range(WAVES[0], WAVES[1]):
        dispatch[r].start()
    land[0] = send[0]
    sel[...] = picked.T.astype(BF)

    def rows_of(k):
        return pl.ds(bounds[k], bounds[k + 1] - bounds[k])

    low, high = pl.ds(0, half), pl.ds(half, half)
    all_cols = pl.ds(0, width)

    def gather_copy(k, j, src, dst, cols, device):
        return remote(
            xbuf.at[src, rows_of(k), cols], xbuf.at[dst, rows_of(k), cols],
            as_sem.at[k, j], ar_sem.at[k, j], (me_n, device),
        )

    gather = [
        (
            gather_copy(k, 0, OWN, LEFT, all_cols, to_right),
            gather_copy(k, 1, OWN, RIGHT, all_cols, to_left),
            gather_copy(k, 2, LEFT, OPP, low, to_right),
            gather_copy(k, 3, RIGHT, OPP, high, to_left),
            gather_copy(k, 4, OWN, 4 + OWN, all_cols, to_core),
            gather_copy(k, 5, LEFT, 4 + LEFT, all_cols, to_core),
            gather_copy(k, 6, RIGHT, 4 + RIGHT, all_cols, to_core),
            gather_copy(k, 7, OPP, 4 + OPP, all_cols, to_core),
        )
        for k in range(chunks)
    ]

    def spread(rows, row0, slots, slot0):
        at = lax.broadcasted_iota(jnp.int32, (rows, slots), 0) + row0
        frm = lax.broadcasted_iota(jnp.int32, (rows, slots), 1) + slot0
        same = at == CAP * (frm // PAD) + frm % PAD
        return (same & (frm % PAD < CAP)).astype(BF)

    arrived = [0]
    gate_copies = []

    def share_gates(k, pack, got):
        flat = jnp.dot(pack, got, preferred_element_type=F32).astype(BF)
        packed = jnp.zeros((PAD, 128), F32)
        e_at = lax.broadcasted_iota(jnp.int32, (128, 128), 0)
        l_at = lax.broadcasted_iota(jnp.int32, (128, 128), 1)
        for t in range(TILES[k]):
            move = ((e_at < experts) & (l_at == experts * t + e_at)).astype(BF)
            packed = packed + jnp.dot(
                flat[t * PAD : (t + 1) * PAD], move, preferred_element_type=F32
            )
        gp[k, 0] = packed.astype(BF)
        copies = []
        for dx, there in ((0, OWN), (1, LEFT), (3, RIGHT), (2, OPP)):
            for dc in (0, 1):
                if (dx, dc) == (0, 0):
                    continue
                n = len(copies)
                copy = remote(
                    gp.at[k, 0], gp.at[k, 4 * dc + there], gs_sem.at[k, n], gr_sem.at[k, n],
                    (me_n, dev_at(dx, dc)),
                )
                copy.start()
                copies.append(copy)
        gate_copies.append(copies)

    def deliver(k):
        lo, hi = bounds[k], bounds[k + 1]
        first, last = lo // CAP, min(N_OFF, (hi - 1) // CAP + 1)
        while arrived[0] < last - 1:
            arrived[0] += 1
            dispatch[arrived[0]].wait_recv()
        if k + 2 < len(WAVES):
            for r in range(WAVES[k + 1], WAVES[k + 2]):
                dispatch[r].start()
        pack = spread(hi - lo, lo, (last - first) * PAD, first * PAD)
        share_gates(k, pack, land[first:last, :, width:].reshape((last - first) * PAD, 128))

        def body(i, carry):
            cols = pl.ds(pl.multiple_of(i * step, step), step)
            got = land[first:last, :, cols].reshape((last - first) * PAD, step)
            xbuf[OWN, lo:hi, cols] = jnp.dot(pack, got, preferred_element_type=F32).astype(BF)
            return carry

        lax.fori_loop(0, width // step, body, 0, unroll=5)
        for j in (0, 1, 4):
            gather[k][j].start()

    def relay(k):
        gather[k][0].wait_recv()
        gather[k][2].start()
        gather[k][5].start()
        gather[k][1].wait_recv()
        gather[k][3].start()
        gather[k][6].start()

    def relay_opp(k):
        gather[k][2].wait_recv()
        gather[k][3].wait_recv()
        gather[k][7].start()

    def hidden(k):
        lo, hi = bounds[k], bounds[k + 1]
        m = 8 * (hi - lo)
        for j in (4, 5, 6, 7):
            gather[k][j].wait_recv()
        for copy in gate_copies[k]:
            copy.wait_recv()
        contract = (((1,), (1,)), ((), ()))
        columns = []
        for e in range(experts):
            pieces = []
            for s in range(8):
                for t in range(TILES[k]):
                    at = experts * t + e
                    pieces.append(gp[k, s, :, at : at + 1].astype(F32))
            columns.append(jnp.concatenate(pieces, axis=0))
        for e in range(experts):
            rows = xbuf[:, lo:hi, :].reshape(m, width)
            gate_val = lax.dot_general(rows, wg[e], contract, preferred_element_type=F32)
            up_val = lax.dot_general(rows, wu[e], contract, preferred_element_type=F32)
            act = gate_val / (1.0 + jnp.exp(-gate_val)) * up_val
            hid[e, 0:m, :] = (act * columns[e]).astype(BF)

    def reduce_copy(k, j, src, dst, cols, device, n=None):
        return remote(
            src.at[rows_of(k), cols], dst.at[rows_of(k), cols],
            rs_sem.at[k, j], rr_sem.at[k, j], (me_n, device),
        )

    reduce = [
        (
            remote(
                xbuf.at[4:8, rows_of(k), low], prbuf.at[:, rows_of(k), low],
                rs_sem.at[k, 0], rr_sem.at[k, 0], (me_n, to_core),
            ),
            remote(
                xbuf.at[4:8, rows_of(k), high], prbuf.at[:, rows_of(k), high],
                rs_sem.at[k, 1], rr_sem.at[k, 1], (me_n, to_core),
            ),
            reduce_copy(k, 2, xbuf.at[OPP, :, low], rabuf, low, to_right),
            reduce_copy(k, 3, xbuf.at[OPP, :, high], rbbuf, low, to_left),
            reduce_copy(k, 4, xbuf.at[RIGHT], flbuf, high, to_right),
            reduce_copy(k, 5, xbuf.at[LEFT], frbuf, low, to_left),
            reduce_copy(k, 6, xbuf.at[RIGHT], flbuf, low, to_right),
            reduce_copy(k, 7, xbuf.at[LEFT], frbuf, high, to_left),
        )
        for k in range(chunks)
    ]

    def project(k):
        lo, hi = bounds[k], bounds[k + 1]
        m = 8 * (hi - lo)
        for j in range(8):
            gather[k][j].wait_send()

        def body(i, carry):
            cols = pl.ds(pl.multiple_of(i * step, step), step)
            total = jnp.dot(hid[0, 0:m, :], wd[0, :, cols], preferred_element_type=F32)
            for e in range(1, experts):
                total += jnp.dot(hid[e, 0:m, :], wd[e, :, cols], preferred_element_type=F32)
            xbuf[:, lo:hi, cols] = total.astype(BF).reshape(8, hi - lo, step)
            return carry

        lax.fori_loop(0, half // step, body, 0)
        reduce[k][0].start()
        lax.fori_loop(half // step, width // step, body, 0)
        reduce[k][1].start()

    def add_up(k, place, start, others):
        lo, hi = bounds[k], bounds[k + 1]

        def body(i, carry):
            at = pl.multiple_of(i * step, step)
            cols = pl.ds(start + at, step)
            total = xbuf[place, lo:hi, cols].astype(F32)
            for other, shift in others:
                total += other[lo:hi, pl.ds(at + shift, step)].astype(F32)
            xbuf[place, lo:hi, cols] = total.astype(BF)
            return carry

        lax.fori_loop(0, half // step, body, 0)

    def pass_on(k):
        reduce[k][0].wait_recv()
        add_up(k, OPP, 0, ((prbuf.at[OPP], 0),))
        reduce[k][2].start()
        reduce[k][1].wait_recv()
        add_up(k, OPP, half, ((prbuf.at[OPP], half),))
        reduce[k][3].start()
        add_up(k, RIGHT, half, ((prbuf.at[RIGHT], half),))
        reduce[k][4].start()
        add_up(k, LEFT, 0, ((prbuf.at[LEFT], 0),))
        reduce[k][5].start()

    def pass_home(k):
        reduce[k][2].wait_recv()
        add_up(k, RIGHT, 0, ((prbuf.at[RIGHT], 0), (rabuf, 0)))
        reduce[k][6].start()
        reduce[k][3].wait_recv()
        add_up(k, LEFT, half, ((prbuf.at[LEFT], half), (rbbuf, 0)))
        reduce[k][7].start()

    returns = [None]
    returned = [0]

    def give_back(k):
        lo, hi = bounds[k], bounds[k + 1]
        for j in (4, 5, 6, 7):
            reduce[k][j].wait_recv()
        for start in (0, half):
            add_up(k, OWN, start, ((prbuf.at[OWN], start), (flbuf, start), (frbuf, start)))
        first, last = returned[0], hi // CAP
        returned[0] = last
        row0 = first * CAP // PAD * PAD
        unpack = (
            lax.broadcasted_iota(jnp.int32, ((last - first) * PAD, hi - row0), 1) + row0
        )
        frm = lax.broadcasted_iota(jnp.int32, ((last - first) * PAD, hi - row0), 0) + first * PAD
        unpack = ((unpack == CAP * (frm // PAD) + frm % PAD) & (frm % PAD < CAP)).astype(BF)
        own = 1 if first == 0 else 0

        def body(i, carry):
            cols = pl.ds(pl.multiple_of(i * step, step), step)
            back = jnp.dot(unpack, xbuf[OWN, row0:hi, cols], preferred_element_type=F32)
            back = back.astype(BF).reshape(last - first, PAD, step)
            if own:
                ret[0, :, cols] = back[0]
            send[first + own : last, :, cols] = back[own:]
            return carry

        lax.fori_loop(0, width // step, body, 0, unroll=5)
        for r in range(first + own, last):
            dz, dy = OFFS[r]
            copy = remote(
                send.at[r, :, all_cols], ret.at[r], bs_sem.at[r], br_sem.at[r],
                (node_at(-dz, -dy), me_d),
            )
            copy.start()
            returns.append(copy)

    deliver(0)
    relay(0)
    deliver(1)
    relay_opp(0)
    for load in loads:
        load.wait()
    hidden(0)
    project(0)
    pass_on(0)
    relay(1)
    deliver(2)
    pass_home(0)
    deliver(3)
    relay_opp(1)
    hidden(1)
    project(1)
    relay(2)
    pass_on(1)
    for r in range(1, N_OFF):
        dispatch[r].wait_send()
    give_back(0)
    relay(3)
    relay_opp(2)
    hidden(2)
    pass_home(1)
    project(2)
    pass_on(2)
    relay_opp(3)
    give_back(1)
    hidden(3)
    project(3)
    pass_on(3)
    pass_home(2)
    pass_home(3)
    give_back(2)
    give_back(3)

    for r in range(1, N_OFF):
        returns[r].wait_recv()
    outs = []
    parts = 2
    for p in range(parts):

        def combine(i, carry, p=p):
            cols = pl.ds(pl.multiple_of(p * (width // parts) + i * step, step), step)
            got = ret[:, :, cols].reshape(slots_all, step)
            total[:, cols] = jnp.dot(sel[...], got, preferred_element_type=F32).astype(BF)
            return carry

        lax.fori_loop(0, width // parts // step, combine, 0, unroll=5)
        cols = pl.ds(p * (width // parts), width // parts)
        copy = pltpu.make_async_copy(total.at[:, cols], out_ref.at[:, cols], o_sem.at[p])
        copy.start()
        outs.append(copy)

    for copies in gate_copies:
        for copy in copies:
            copy.wait_send()
    for k in range(chunks):
        for copy in reduce[k]:
            copy.wait_send()
    for r in range(1, N_OFF):
        returns[r].wait_send()
    for copy in outs:
        copy.wait()


def shards(tokens, node_ids, expert_pick, gate_share, gate_proj, up_proj, down_proj):
    toks, width = tokens.shape
    experts, units, _ = gate_proj.shape
    half = width // 2
    chunks = len(TILES)
    vmem = pl.BlockSpec(memory_space=pltpu.VMEM)
    hbm = pl.BlockSpec(memory_space=pl.ANY)
    dma = pltpu.SemaphoreType.DMA
    weights = pltpu.VMEM((experts, units, width), BF)
    return pl.pallas_call(
        kernel,
        out_shape=jax.ShapeDtypeStruct((toks, width), BF),
        in_specs=[vmem] * 4 + [hbm] * 3,
        out_specs=hbm,
        scratch_shapes=[
            weights,
            weights,
            weights,
            pltpu.VMEM((8, ROWS, width), BF),
            pltpu.VMEM((4, ROWS, width), BF),
            pltpu.VMEM((ROWS, half), BF),
            pltpu.VMEM((ROWS, half), BF),
            pltpu.VMEM((ROWS, width), BF),
            pltpu.VMEM((ROWS, width), BF),
            pltpu.VMEM((N_OFF, PAD, width + 128), BF),
            pltpu.VMEM((N_OFF, PAD, width + 128), BF),
            pltpu.VMEM((N_OFF, PAD, width), BF),
            pltpu.VMEM((experts, 8 * PAD * max(TILES), units), BF),
            pltpu.VMEM((chunks, 8, PAD, 128), BF),
            pltpu.VMEM((toks, N_OFF * PAD), BF),
            pltpu.VMEM((toks, width), BF),
            dma((2,)),
            dma((3,)),
            dma((N_OFF,)),
            dma((N_OFF,)),
            dma((chunks, 7)),
            dma((chunks, 7)),
            dma((chunks, 8)),
            dma((chunks, 8)),
            dma((chunks, 8)),
            dma((chunks, 8)),
            dma((N_OFF,)),
            dma((N_OFF,)),
        ],
        compiler_params=pltpu.CompilerParams(
            collective_id=0, has_side_effects=True, vmem_limit_bytes=67043328
        ),
    )(tokens, node_ids.T, expert_pick.T, gate_share.T, gate_proj, up_proj, down_proj)


def solution(mesh):
    return jax.shard_map(
        shards,
        mesh=mesh,
        in_specs=(
            P(("node", "dev"), None),
            P(("node", "dev"), None),
            P(("node", "dev"), None),
            P(("node", "dev"), None),
            P("node", "dev", None),
            P("node", "dev", None),
            P("node", "dev", None),
        ),
        out_specs=P(("node", "dev"), None),
        check_vma=False,
    )
```
